256 devices in a mesh: grp: 2 (over z), pool: 128 (over y, x, core).
Axes of the slice: x: 8, y: 8, z: 2, core: 2. Of those that a mesh axis runs over, the one named last changes fastest.
The devices are a block of a 8x8x16 slice.
Arguments:
- query: bfloat16 [256, 4096], P(('grp', 'pool')), parts along dimension 0, may hold values from -6 to 6
- kv_pool: bfloat16 [16384, 2, 16, 512], P(('grp', 'pool')), parts along dimension 0, may hold values from -6 to 6
- holder_table: int32 [256, 128], P(('grp', 'pool')), parts along dimension 0, may hold values from 0 to 127, as said below
- slot_table: int32 [256, 128], P(('grp', 'pool')), parts along dimension 0, may hold values from 0 to 63
- lengths: int32 [256], P(('grp', 'pool')), parts along dimension 0, may hold values from 96 to 128, as said below
- out_weight: bfloat16 [4096, 8192], P('pool'), may hold values from -5 to 5
Outputs:
- mixed: bfloat16 [256, 8192], P(('grp', 'pool')), parts along dimension 0
The draws below stay inside these ranges and needn't reach their ends.
There are 2 independent parts, one for each index of `grp`. The reference program is written for one: setup_inputs(seed, part) draws one part's arguments, and reference() takes and returns one part's arrays. A program takes and returns all parts, laid end to end along the dimension named above; an argument that names none is the same for every part. Nothing has to cross between parts.
Inputs may be any that keep to these rules, and one draw needn't show every extreme that they name: `holder_table`: entry [r, j] is the index along pool of the device holding block j of request r. Of one request's 128 blocks at most 2 have the same holder, and some holder has exactly 2 of the request's first 96 blocks. Request r's live blocks are 0 to lengths[r] - 1; some request has 128.
All inputs are finite; a program needn't handle non-finite values.
Results may differ from the reference program's by a relative error of at most 0.0053.
Values may be sent and summed in bfloat16 or wider, within the bound.
No kernel may reach another device: no remote copies, remote signals or barrier semaphores. Data moves between devices by JAX's collectives and lax.ppermute only.
A program may use at most 64 MiB of HBM per device.

```python
import math
import jax
import jax.numpy as jnp
from jax import lax

H = 32
KVH = 4
HD = 128
D = 8192
BLK = 16
MAXB = 128
MINB = 96
SLOTS_DEV = 64
REQUESTS = 128
CAP = 2
N_POOL = 128


def draw_query(key, part):
    groups = H // KVH
    result = jnp.clip(jax.random.normal(jax.random.fold_in(key, 11), (REQUESTS, KVH, groups, HD), jnp.float32), -6.0, 6.0)
    return result.reshape(REQUESTS, H * HD).astype(jnp.bfloat16)


def draw_kv_pool(key, part):
    slot_total = N_POOL * SLOTS_DEV
    result = jnp.clip(jax.random.normal(jax.random.fold_in(key, 21), (slot_total, 2, BLK, KVH, HD), jnp.float32), -6.0, 6.0)
    return result.reshape(slot_total, 2, BLK, KVH * HD).astype(jnp.bfloat16)


def draw_holder_table(key, part):
    spare = (N_POOL - 1) * CAP

    def one_request(request_key):
        home = jax.random.randint(jax.random.fold_in(request_key, 1), (), 0, N_POOL)
        spread = jnp.arange(spare, dtype=jnp.int32)
        others = (home + 1 + spread // CAP) % N_POOL
        order = jax.random.permutation(jax.random.fold_in(request_key, 2), spare)
        picked = others[order][:MAXB - CAP]
        combined = jnp.concatenate([jnp.zeros((CAP,), jnp.int32) + home, picked])
        head_order = jax.random.permutation(jax.random.fold_in(request_key, 3), MINB)
        tail_order = jax.random.permutation(jax.random.fold_in(request_key, 4), MAXB - MINB)
        return jnp.concatenate([combined[:MINB][head_order], combined[MINB:][tail_order]]).astype(jnp.int32)
    return jax.vmap(one_request)(jax.random.split(jax.random.fold_in(key, 31), REQUESTS))


def draw_lengths(key, part):
    result = jax.random.randint(jax.random.fold_in(key, 41), (REQUESTS,), MINB, MAXB + 1)
    longest = jax.random.randint(jax.random.fold_in(key, 43), (), 0, REQUESTS)
    return jnp.where(jnp.arange(REQUESTS, dtype=jnp.int32) == longest, MAXB, result).astype(jnp.int32)


def with_ends(values, rng, smallest, top_value):
    longest = values.shape.index(max(values.shape))
    spots = []
    for shift in (0, 1):
        where = [jax.random.randint(jax.random.fold_in(rng, axis), (), 0, length) for axis, length in enumerate(values.shape)]
        where[longest] = (where[longest] + shift) % values.shape[longest]
        spots.append(tuple(where))
    return values.at[spots[0]].set(smallest).at[spots[1]].set(top_value)


def strengthened(array, key, source, target, shards_of, factor):
    owner, partner = [(jnp.arange(array.shape[position]) // (array.shape[position] // shards_of)).reshape([-1 if axis == position else 1 for axis in range(array.ndim)]) for position in (source, target)]
    chosen = jax.random.permutation(key, shards_of)[partner]
    strong = (owner == chosen) | (owner == (partner + shards_of // 2) % shards_of)
    return jnp.where(strong, factor * array, array)


def levels(key, shape, pieces, least, top_value):
    def one(dim, shards_of):
        heights = jax.random.uniform(jax.random.fold_in(jax.random.fold_in(key, 6), dim), (shards_of,), jnp.float32, least / len(pieces), top_value / len(pieces))
        return jnp.repeat(jnp.exp(heights), shape[dim] // shards_of).reshape((-1,) + (1,) * (len(shape) - dim - 1))

    loudness = one(*pieces[0])
    for cut in pieces[1:]:
        loudness = loudness * one(*cut)
    return loudness


def heavy_noise(rng, extent, scale, bound, pieces, heavy, kind=jnp.bfloat16):
    array = scale * jax.random.normal(rng, extent, jnp.float32)
    if pieces:
        array = array * levels(rng, extent, pieces, -0.22, 0.18)
    return jnp.clip(strengthened(array, jax.random.fold_in(rng, 3), *heavy), -bound, bound).astype(kind)


def setup_inputs(seed: int = 0, part: int = 0) -> dict:
    keys = jax.random.split(jax.random.key(seed), 7)
    part_splits = jax.random.split(jax.random.fold_in(keys[6], part), 7)
    query = draw_query(jax.random.fold_in(jax.random.fold_in(keys[6], part), 71), part)
    kv_pool = draw_kv_pool(jax.random.fold_in(jax.random.fold_in(keys[6], part), 71), part)
    holder_table = draw_holder_table(jax.random.fold_in(jax.random.fold_in(keys[6], part), 71), part)
    slot_table = with_ends(jax.random.randint(part_splits[3], (REQUESTS, MAXB), 0, SLOTS_DEV), jax.random.fold_in(part_splits[3], 1), 0, SLOTS_DEV - 1).astype(jnp.int32)
    lengths = draw_lengths(jax.random.fold_in(jax.random.fold_in(keys[6], part), 71), part)
    out_weight = heavy_noise(keys[5], (H * HD, D), 0.2, 5.0, ((0, 128),), (0, 1, 128, 5.5))
    return dict(query=query, kv_pool=kv_pool, holder_table=holder_table, slot_table=slot_table, lengths=lengths, out_weight=out_weight)


lowest = -1e+30

def request_attention(query_heads, block_keys, block_values, live_blocks):
    scores = jnp.einsum('gqd,jbgd->jgqb', query_heads.astype(jnp.float32), block_keys.astype(jnp.float32))
    scores = scores * (1.0 / math.sqrt(HD))
    maxima = lax.optimization_barrier(jnp.max(scores, axis=-1))
    shifted = jnp.exp(scores - maxima[..., None])
    totals = lax.optimization_barrier(jnp.sum(shifted, axis=-1))
    rounded = lax.optimization_barrier(shifted.astype(jnp.bfloat16))
    outputs = jnp.einsum('jgqb,jbgd->jgqd', rounded.astype(jnp.float32), block_values.astype(jnp.float32))
    live_wide = live_blocks[:, None, None]
    peak_score = lax.optimization_barrier(jnp.max(jnp.where(live_wide, maxima, lowest), axis=0))
    factor = jnp.exp(jnp.where(live_wide, maxima - peak_score[None], lowest))
    numerator = lax.optimization_barrier(jnp.sum(factor[..., None] * outputs, axis=0))
    denominator = lax.optimization_barrier(jnp.sum(factor * totals, axis=0))
    return numerator / denominator[..., None]

def reference(query, kv_pool, holder_table, slot_table, lengths, out_weight):

    def one_request(inputs):
        query_row, holders, slot_ids, length = inputs
        pool_rows = holders * SLOTS_DEV + slot_ids
        blocks = kv_pool[pool_rows]
        block_keys = blocks[:, 0].reshape(MAXB, BLK, KVH, HD)
        block_values = blocks[:, 1].reshape(MAXB, BLK, KVH, HD)
        live_blocks = jnp.arange(MAXB, dtype=jnp.int32) < length
        result = request_attention(query_row.reshape(KVH, H // KVH, HD), block_keys, block_values, live_blocks)
        return result.reshape(H * HD).astype(jnp.bfloat16)
    attention = lax.map(one_request, (query, holder_table, slot_table, lengths))
    return jnp.dot(attention, out_weight, preferred_element_type=jnp.float32).astype(jnp.bfloat16)
```

```python
import functools
import math

import jax
import jax.numpy as jnp
from jax import lax
from jax.experimental import pallas as pl
from jax.experimental.pallas import tpu as pltpu
from jax.sharding import Mesh
from jax.sharding import PartitionSpec as P

H = 32
KVH = 4
HD = 128
GROUPS = H // KVH
POOL = ("y", "x", "c")
GRP_POOL = ("grp", "y", "x", "c")
LOWEST = -1e30
RATE = math.log2(math.e) / math.sqrt(HD)
TWICE = math.log(2.0) * math.sqrt(HD)
NUM = H * HD
WIDE = NUM + HD

INTERPRET = False

f32 = jnp.float32
bf16 = jnp.bfloat16


def call(body, outs, *args, scalars=(), scratch=(), mib=6):
    smem = pl.BlockSpec(memory_space=pltpu.SMEM)
    vmem = pl.BlockSpec(memory_space=pltpu.VMEM)
    return pl.pallas_call(
        body,
        out_shape=outs,
        in_specs=[smem] * len(scalars) + [vmem] * len(args),
        out_specs=jax.tree.map(lambda _: vmem, outs),
        scratch_shapes=list(scratch),
        compiler_params=pltpu.CompilerParams(vmem_limit_bytes=mib << 20),
        interpret=INTERPRET,
    )(*scalars, *args)


def shifted(v, axis, k):
    n = lax.axis_size(axis)
    return lax.ppermute(v, axis, [(i, (i + k) % n) for i in range(n)])


def swapped(v):
    return lax.ppermute(v, "c", [(0, 1), (1, 0)])


def shifted_xc(v, k, flip):
    nx, nc = lax.axis_size("x"), lax.axis_size("c")
    perm = [(i * nc + j, ((i + k) % nx) * nc + (j ^ flip)) for i in range(nx) for j in range(nc)]
    return lax.ppermute(v, ("x", "c"), perm)


def attention_body(me_ref, own_ref, other_ref, kv_ref, keep_ref, send_ref, q_scr, s_scr, p_scr, stat_scr):
    g = pl.program_id(0)
    half = own_ref.shape[0]
    rows = 2 * half
    slots, _, blk, _ = kv_ref.shape
    tokens = slots * blk

    @pl.when(g == 0)
    def _():
        lane = lax.broadcasted_iota(jnp.int32, (half, HD), 1)
        slot_lane = jnp.where(lane < slots, lane, lane - slots).astype(f32)
        me = me_ref[0].astype(f32)
        twice_hi = jnp.asarray(TWICE, f32).astype(bf16).astype(f32)
        twice_lo = TWICE - twice_hi
        for i, ref in enumerate((own_ref, other_ref)):
            holder = ref[:, NUM : NUM + HD].astype(f32)
            slot = ref[:, NUM + HD : NUM + 2 * HD].astype(f32)
            hit = holder == me
            first = jnp.min(jnp.where(hit, slot, 999.0), axis=1, keepdims=True)
            last = jnp.max(jnp.where(hit, slot, -1.0), axis=1, keepdims=True)
            count = jnp.sum(jnp.where(hit, 1.0, 0.0), axis=1, keepdims=True)
            used = (slot_lane == first) | (slot_lane == last)
            double = used & (first == last) & (count > 1.5)
            high = jnp.where(used, jnp.where(double, twice_hi, 0.0), LOWEST)
            low = jnp.where(double, twice_lo, 0.0)
            bias = jnp.where(lane < slots, high, low).astype(bf16)
            for h in range(GROUPS):
                q_scr[pl.ds(h * rows + i * half, half), HD:] = bias
        stat_scr[...] = jnp.zeros_like(stat_scr)

    for h in range(GROUPS):
        cols = pl.ds(pl.multiple_of(g * (GROUPS * HD) + h * HD, HD), HD)
        q_scr[pl.ds(h * rows, half), :HD] = own_ref[:, cols]
        q_scr[pl.ds(h * rows + half, half), :HD] = other_ref[:, cols]
    token_slot = lax.broadcasted_iota(jnp.int32, (tokens, HD), 0) // blk
    lane = lax.broadcasted_iota(jnp.int32, (tokens, HD), 1)
    hot = jnp.where(jnp.where(lane < slots, lane, lane - slots) == token_slot, 1.0, 0.0).astype(bf16)
    keys = jnp.concatenate([kv_ref[:, 0].reshape(tokens, HD), hot], axis=1)
    values = jnp.concatenate([kv_ref[:, 1].reshape(tokens, HD), jnp.ones((tokens, HD), bf16)], axis=1)
    s_scr[...] = lax.dot_general(q_scr[...], keys, (((1,), (1,)), ((), ())), preferred_element_type=f32)

    step = 64
    stat_lane = lax.broadcasted_iota(jnp.int32, (step, HD), 1)
    def block(i, carry):
        at = pl.ds(pl.multiple_of(i * step, step), step)
        s = s_scr[at, :]
        top = jnp.max(s, axis=1, keepdims=True).astype(bf16).astype(f32)
        p_scr[at, :] = jnp.exp2((s - top) * RATE).astype(bf16)
        head = g * GROUPS + (i * step) // rows
        here = pl.ds(pl.multiple_of((i * step) % rows, step), step)
        stat_scr[here, :] = jnp.where(stat_lane == head, top, stat_scr[here, :])
        return carry
    lax.fori_loop(0, GROUPS * rows // step, block, 0)

    for h in range(GROUPS):
        out = jnp.dot(p_scr[pl.ds(h * rows, rows), :], values, preferred_element_type=f32)
        cols = pl.ds(pl.multiple_of(g * (GROUPS * HD) + h * HD, HD), HD)
        keep_ref[:, cols] = out[:half, :HD]
        send_ref[:, cols] = out[half:, :HD].astype(bf16)
        total = out[:, HD:]
        high = total.astype(bf16).astype(f32)
        all_lane = lax.broadcasted_iota(jnp.int32, (rows, HD), 1)
        head = g * GROUPS + h
        stat = jnp.where(all_lane == head + H, high, stat_scr[...])
        stat_scr[...] = jnp.where(all_lane == head + 2 * H, total - high, stat)

    @pl.when(g == pl.num_programs(0) - 1)
    def _():
        keep_ref[:, NUM:] = stat_scr[:half, :]
        send_ref[:, NUM:] = stat_scr[half:, :].astype(bf16)


def attention_partials(me, own, other, kv_pool):
    half = own.shape[0]
    slots, _, blk, _ = kv_pool.shape
    rows, tokens = 2 * half, slots * blk
    whole = lambda shape: pl.BlockSpec(shape, lambda g: (0,) * len(shape))
    return pl.pallas_call(
        attention_body,
        grid=(KVH,),
        out_shape=(jax.ShapeDtypeStruct((half, WIDE), f32), jax.ShapeDtypeStruct((half, WIDE), bf16)),
        in_specs=[
            pl.BlockSpec(memory_space=pltpu.SMEM),
            whole(own.shape),
            whole(other.shape),
            pl.BlockSpec((slots, 2, blk, HD), lambda g: (0, 0, 0, g)),
        ],
        out_specs=(whole((half, WIDE)), whole((half, WIDE))),
        scratch_shapes=[
            pltpu.VMEM((GROUPS * rows, 2 * HD), bf16),
            pltpu.VMEM((GROUPS * rows, tokens), f32),
            pltpu.VMEM((GROUPS * rows, tokens), bf16),
            pltpu.VMEM((rows, HD), f32),
        ],
        cost_estimate=pl.CostEstimate(flops=4 * KVH * GROUPS * rows * tokens * 2 * HD, transcendentals=0, bytes_accessed=0),
        compiler_params=pltpu.CompilerParams(dimension_semantics=("arbitrary",), vmem_limit_bytes=28 << 20),
        interpret=INTERPRET,
    )(me, own, other, kv_pool)


def lanes_at(stat, part):
    return pltpu.roll(stat, HD - part * H, 1) if part else stat


def merge_stats(stats):
    top = functools.reduce(jnp.maximum, stats)
    factors = [jnp.exp2((s - top) * RATE) for s in stats]
    total = sum(f * (lanes_at(s, 1) + lanes_at(s, 2)) for f, s in zip(factors, stats))
    return top, factors, total


def packed_stats(top, total):
    lane = lax.broadcasted_iota(jnp.int32, top.shape, 1)
    high = total.astype(bf16).astype(f32)
    low = total - high
    zero = jnp.zeros_like(top)
    return jnp.where(
        lane < H,
        top,
        jnp.where(
            lane < 2 * H, pltpu.roll(high, H, 1), jnp.where(lane < 3 * H, pltpu.roll(low, 2 * H, 1), zero)
        ),
    )


def merged_head(factors, pieces, h):
    cols = slice(h * HD, (h + 1) * HD)
    return sum(f[:, h : h + 1] * p[:, cols].astype(f32) for f, p in zip(factors, pieces))


def merge_core_body(keep_ref, got_ref, *out_refs):
    step = keep_ref.shape[0] // len(out_refs)
    for i, out_ref in enumerate(out_refs):
        at = pl.ds(i * step, step)
        pieces = [keep_ref.at[at, :], got_ref.at[at, :]]
        top, factors, total = merge_stats([p[:, NUM:].astype(f32) for p in pieces])
        for h in range(H):
            out_ref[:, h * HD : (h + 1) * HD] = merged_head(factors, pieces, h).astype(out_ref.dtype)
        out_ref[:, NUM:] = packed_stats(top, total).astype(out_ref.dtype)


def merge_x_body(n, y_ref, *refs):
    pieces, outs, scr = refs[:n], refs[n:-1], refs[-1]
    y = y_ref[0]
    top, factors, total = merge_stats([p[:, NUM:].astype(f32) for p in pieces])
    for h in range(H):
        scr[:, h * HD : (h + 1) * HD] = merged_head(factors, pieces, h)
    stat = packed_stats(top, total)
    ny = len(outs)
    width = NUM // ny
    heads = H // ny
    for k, out_ref in enumerate(outs):
        to = lax.rem(y + k, ny)
        out_ref[:, :width] = scr[:, pl.ds(pl.multiple_of(to * width, width), width)].astype(out_ref.dtype)
        out_ref[:, width:] = pltpu.roll(stat, lax.rem(HD - to * heads, HD), 1).astype(out_ref.dtype)


def merge_y_body(*refs):
    pieces, out_ref = refs[:-1], refs[-1]
    width = out_ref.shape[1]
    got = [p[...].astype(f32) for p in pieces]
    got = [pltpu.roll(v, k, 0) if k else v for k, v in enumerate(got)]
    _, factors, total = merge_stats([v[:, width:] for v in got])
    for h in range(width // HD):
        numer = merged_head(factors, got, h)
        out_ref[:, h * HD : (h + 1) * HD] = (numer / total[:, h : h + 1]).astype(bf16)


def weight_pack_body(pos_ref, mine_ref, got_ref, *out_refs):
    x, c = pos_ref[0], pos_ref[1]
    nx = len(out_refs)
    depth, half = got_ref.shape
    width = half // nx
    for k, out_ref in enumerate(out_refs):
        to = lax.rem(x + k, nx)
        mine = mine_ref[:, pl.ds(pl.multiple_of(c * half + to * width, width), width)]
        got = got_ref[:, pl.ds(pl.multiple_of(to * width, width), width)]
        out_ref[pl.ds(pl.multiple_of(c * depth, depth), depth), :] = mine
        out_ref[pl.ds(pl.multiple_of((1 - c) * depth, depth), depth), :] = got


def project_body(n, nc, pos_ref, *refs):
    weights, rows, keep_ref, outs = refs[:n], refs[n : n + n * nc], refs[n + n * nc], refs[n + n * nc + 1 : -1]
    w_scr = refs[-1]
    x = pos_ref[0]
    depth = weights[0].shape[0]
    for k, w in enumerate(weights):
        at = lax.rem(x + (n - k), n)
        w_scr[pl.ds(pl.multiple_of(at * depth, depth), depth), :] = w[...]
    a = jnp.concatenate([r[...] for r in rows], axis=0)
    total, ny = a.shape[0], len(outs) + 1
    inner = total // ny
    i = lax.broadcasted_iota(jnp.int32, (total, total), 0)
    j = lax.broadcasted_iota(jnp.int32, (total, total), 1)
    turn = jnp.where(j == lax.rem(i, inner) * ny + i // inner, 1.0, 0.0).astype(bf16)
    a = jnp.dot(turn, a, preferred_element_type=f32).astype(bf16)
    out = jnp.dot(a, w_scr[...], preferred_element_type=f32)
    keep_ref[...] = out[:inner]
    for k, o in enumerate(outs):
        o[...] = out[(k + 1) * inner : (k + 2) * inner].astype(bf16)


def sum_body(n, *refs):
    pieces, outs = refs[:n], refs[n:]
    total = sum(p[...].astype(f32) for p in pieces).astype(bf16)
    for i, o in enumerate(outs):
        o[...] = total[i : i + 1]


def place_body(nx, nc, pos_ref, *refs):
    pieces, out_ref = refs[:-1], refs[-1]
    x, c = pos_ref[0], pos_ref[1]
    width = pieces[0].shape[1]
    for kx in range(nx):
        for kc in range(nc):
            core = c if kc == 0 else 1 - c
            at = (core * nx + lax.rem(x + kx, nx)) * width
            out_ref[:, pl.ds(pl.multiple_of(at, width), width)] = pieces[kx * nc + kc][...]


def per_device(query, kv_pool, holder_table, slot_table, lengths, out_weight):
    ny, nx, nc = (lax.axis_size(a) for a in POOL)
    y, x, c = (lax.axis_index(a) for a in POOL)
    me = jnp.reshape((y * nx + x) * nc + c, (1,)).astype(jnp.int32)
    y_pos = jnp.reshape(y, (1,)).astype(jnp.int32)
    pos = jnp.stack([x, c]).astype(jnp.int32)
    shape = jax.ShapeDtypeStruct

    live = lax.broadcasted_iota(jnp.int32, holder_table.shape, 1) < lengths[:, None]
    holders = jnp.where(live, holder_table, -1)
    row = jnp.concatenate([query, holders.astype(bf16), slot_table.astype(bf16)], axis=1)
    d_half = out_weight.shape[1] // nc
    depth = out_weight.shape[0]
    w_got = swapped(lax.dynamic_slice(out_weight, (0, (1 - c) * d_half), (depth, d_half)))
    column = jnp.concatenate([row] + [shifted(row, "y", k) for k in range(1, ny)], axis=0)
    column, w_got = lax.optimization_barrier((column, w_got))
    own = jnp.concatenate([column] + [shifted(column, "x", k) for k in range(1, nx)], axis=0)
    other = swapped(own)

    w_outs = call(
        weight_pack_body,
        [shape((nc * depth, d_half // nx), bf16)] * nx,
        out_weight,
        w_got,
        scalars=(pos,),
    )
    other, *w_outs = lax.optimization_barrier((other, *w_outs))
    weights = [w_outs[0]] + [shifted(w_outs[k], "x", k) for k in range(1, nx)]

    keep, send = attention_partials(me, own, other, kv_pool)
    got = swapped(send)
    got, *weights = lax.optimization_barrier((got, *weights))
    parts = call(merge_core_body, [shape((ny, WIDE), bf16)] * nx, keep, got)
    pieces = [parts[0]] + [shifted(parts[k], "x", nx - k) for k in range(1, nx)]
    parts = call(
        functools.partial(merge_x_body, nx),
        [shape((ny, NUM // ny + HD), bf16)] * ny,
        *pieces,
        scalars=(y_pos,),
        scratch=[pltpu.VMEM((ny, NUM), f32)],
    )
    pieces = [parts[0]] + [shifted(parts[k], "y", k) for k in range(1, ny)]
    attention = call(merge_y_body, shape((ny, NUM // ny), bf16), *pieces)

    rows = []
    for kx in range(nx):
        for kc in range(nc):
            rows.append(shifted_xc(attention, kx, kc) if kx or kc else attention)
    width = d_half // nx
    outs = call(
        functools.partial(project_body, nx, nc),
        [shape((nx * nc, width), f32)] + [shape((nx * nc, width), bf16)] * (ny - 1),
        *weights,
        *rows,
        scalars=(pos,),
        scratch=[pltpu.VMEM((nx * nc * depth, width), bf16)],
    )
    pieces = [outs[0]] + [shifted(outs[k], "y", ny - k) for k in range(1, ny)]
    outs = call(functools.partial(sum_body, ny), [shape((1, width), bf16)] * (nx * nc), *pieces)
    pieces = []
    for kx in range(nx):
        for kc in range(nc):
            v = outs[kx * nc + kc]
            pieces.append(shifted_xc(v, (nx - kx) % nx, kc) if kx or kc else v)
    return call(
        functools.partial(place_body, nx, nc), shape((1, out_weight.shape[1]), bf16), *pieces, scalars=(pos,)
    )


def solution(mesh):
    torus = Mesh(mesh.devices.reshape(mesh.shape["grp"], 8, 8, 2), GRP_POOL)
    return jax.shard_map(
        per_device,
        mesh=torus,
        in_specs=(
            P(GRP_POOL, None),
            P(GRP_POOL, None, None, None),
            P(GRP_POOL, None),
            P(GRP_POOL, None),
            P(GRP_POOL),
            P(POOL, None),
        ),
        out_specs=P(GRP_POOL, None),
        check_vma=False,
    )
```

```python
import functools
import math

import jax
import jax.numpy as jnp
from jax import lax
from jax.experimental import pallas as pl
from jax.experimental.pallas import tpu as pltpu
from jax.sharding import Mesh
from jax.sharding import PartitionSpec as P


H = 32
KVH = 4
HD = 128
GROUPS = H // KVH
CORES = 2
POOL = ("y", "x", "c")
CHIPS = ("y", "x")
GRP_POOL = ("grp", "y", "x", "c")
RATE = math.log2(math.e) / math.sqrt(HD)
TWICE = math.log(2.0) * math.sqrt(HD)
UNUSED = -32768.0
HALF = H * HD // CORES
INTERPRET = False

f32 = jnp.float32
bf16 = jnp.bfloat16


def as_product(value):
    pairs = []
    for i in range(128):
        mark = 1.0 + i / 128.0
        unit = 2.0 ** (math.floor(math.log2(value / mark)) - 7)
        bias = round(value / mark / unit) * unit
        pairs.append((abs(mark * bias - value), mark, bias))
    return min(pairs)[1:]


MARK, BIAS = as_product(TWICE)


def attention_body(pos_ref, q_ref, own_ref, other_ref, out_ref, q_scr, k_scr, v_scr, s_scr, p_scr):
    g = pl.program_id(0)
    rows = q_ref.shape[0]
    slots, _, blk, _ = own_ref.shape
    tokens = slots * blk

    @pl.when(g == 0)
    def _():
        me, core = pos_ref[0], pos_ref[1]
        partner = me + 1 - 2 * core
        holder = q_ref[:, HALF : HALF + HD].astype(f32)
        slot = q_ref[:, HALF + HD : HALF + 2 * HD].astype(f32)
        lane = lax.broadcasted_iota(jnp.int32, (rows, HD), 1)
        lane_slot = jnp.where(lane < slots, lane, lane - slots).astype(f32)

        def bias_of(device):
            hit = holder == device.astype(f32)
            first = jnp.min(jnp.where(hit, slot, 999.0), axis=1, keepdims=True)
            last = jnp.max(jnp.where(hit, slot, -1.0), axis=1, keepdims=True)
            count = jnp.sum(jnp.where(hit, 1.0, 0.0), axis=1, keepdims=True)
            used = (lane_slot == first) | (lane_slot == last)
            double = used & (first == last) & (count > 1.5)
            return jnp.where(used, jnp.where(double, BIAS, 0.0), UNUSED)

        bias = jnp.where(lane < slots, bias_of(me), bias_of(partner)).astype(bf16)
        for h in range(GROUPS):
            q_scr[h * rows : (h + 1) * rows, HD:] = bias
        token_slot = lax.broadcasted_iota(jnp.int32, (2 * tokens, HD), 0) // blk
        slot_lane = lax.broadcasted_iota(jnp.int32, (2 * tokens, HD), 1)
        k_scr[:, HD:] = jnp.where(slot_lane == token_slot, MARK, 0.0).astype(bf16)
        v_scr[HD:, :] = jnp.ones((v_scr.shape[0] - HD, 2 * tokens), bf16)

    for h in range(GROUPS):
        cols = pl.ds(pl.multiple_of(g * (GROUPS * HD) + h * HD, HD), HD)
        q_scr[h * rows : (h + 1) * rows, :HD] = q_ref[:, cols]
    for i, ref in enumerate((own_ref, other_ref)):
        at = slice(i * tokens, (i + 1) * tokens)
        k_scr[at, :HD] = ref[:, 0].reshape(tokens, HD)
        v_scr[:HD, at] = ref[:, 1].reshape(tokens, HD).T
    s_scr[...] = lax.dot_general(
        k_scr[...], q_scr[...], (((1,), (1,)), ((), ())), preferred_element_type=f32
    )

    step = 256
    for h in range(GROUPS):
        cols = slice(h * rows, (h + 1) * rows)

        def peak(i, top, cols=cols):
            at = pl.ds(pl.multiple_of(i * step, step), step)
            return jnp.maximum(top, jnp.max(s_scr[at, cols].reshape(step // 8, 8, rows), axis=0))

        top = lax.fori_loop(0, 2 * tokens // step, peak, jnp.full((8, rows), -jnp.inf, f32))
        top = jnp.max(top, axis=0, keepdims=True).astype(bf16).astype(f32)

        def weigh(i, carry, cols=cols, top=top):
            at = pl.ds(pl.multiple_of(i * step, step), step)
            p_scr[at, cols] = jnp.exp2((s_scr[at, cols] - top) * RATE).astype(bf16)
            return carry

        lax.fori_loop(0, 2 * tokens // step, weigh, 0)
        for j in range(4):
            out_ref[dest_of(g, h, j), 32:33, :] = top.astype(bf16)
    out = jnp.dot(v_scr[...], p_scr[...], preferred_element_type=f32)
    for h in range(GROUPS):
        cols = slice(h * rows, (h + 1) * rows)
        total = out[HD : HD + 1, cols]
        high = total.astype(bf16)
        low = (total - high.astype(f32)).astype(bf16)
        for j in range(4):
            dest = dest_of(g, h, j)
            out_ref[dest, 0:32, :] = out[j * 32 : (j + 1) * 32, cols].astype(bf16)
            out_ref[dest, 33:34, :] = high
            out_ref[dest, 34:35, :] = low


def dest_of(g, h, j):
    return ((j % 2) * 4 + g * 2 + h // 4) * 8 + (h % 4) * 2 + j // 2


def attention_partials(pos, q, kv_pool, kv_other, chips):
    rows = q.shape[0]
    slots, _, blk, _ = kv_pool.shape
    tokens = 2 * slots * blk
    steps = KVH // CORES
    whole = lambda shape: pl.BlockSpec(shape, lambda g, pos: (0,) * len(shape))
    out = (chips, 40, rows)
    return pl.pallas_call(
        attention_body,
        grid_spec=pltpu.PrefetchScalarGridSpec(
            num_scalar_prefetch=1,
            grid=(steps,),
            in_specs=[
                whole(q.shape),
                pl.BlockSpec((slots, 2, blk, HD), lambda g, pos: (0, 0, 0, pos[1] * steps + g)),
                pl.BlockSpec((slots, 2, blk, HD), lambda g, pos: (0, 0, 0, g)),
            ],
            out_specs=whole(out),
            scratch_shapes=[
                pltpu.VMEM((GROUPS * rows, 2 * HD), bf16),
                pltpu.VMEM((tokens, 2 * HD), bf16),
                pltpu.VMEM((HD + 16, tokens), bf16),
                pltpu.VMEM((tokens, GROUPS * rows), f32),
                pltpu.VMEM((tokens, GROUPS * rows), bf16),
            ],
        ),
        out_shape=jax.ShapeDtypeStruct(out, bf16),
        cost_estimate=pl.CostEstimate(flops=1 << 34, transcendentals=0, bytes_accessed=0),
        compiler_params=pltpu.CompilerParams(dimension_semantics=("arbitrary",), vmem_limit_bytes=32 << 20),
        interpret=INTERPRET,
    )(pos, q, kv_pool, kv_other)


def merge_body(got_ref, out_ref, f_scr):
    chips, _, rows = got_ref.shape
    peaks = [got_ref[i, 32:33, :].astype(f32) for i in range(chips)]
    top = functools.reduce(jnp.maximum, peaks)
    total = jnp.zeros((1, rows), f32)
    number = jnp.zeros((32, rows), f32)
    for i in range(chips):
        factor = jnp.exp2((peaks[i] - top) * RATE)
        total += factor * (got_ref[i, 33:34, :].astype(f32) + got_ref[i, 34:35, :].astype(f32))
        number += factor * got_ref[i, 0:32, :].astype(f32)
    attention = number / total
    high = attention.astype(bf16)
    out_ref[0:32, :] = high
    out_ref[32:64, :] = (attention - high.astype(f32)).astype(bf16)


def project_body(pos_ref, mine_ref, got_ref, w_ref, w_got_ref, out_ref):
    core = pos_ref[1]
    half = w_got_ref.shape[1]
    left = jnp.concatenate([mine_ref[...], got_ref[...]], axis=0)
    step = 512
    for i in range(half // step):
        cols = pl.ds(pl.multiple_of(core * half + i * step, step), step)
        mine = w_ref[:, cols]
        got = w_got_ref[:, i * step : (i + 1) * step]
        right = jnp.concatenate([mine, mine, got, got], axis=0)
        part = lax.dot_general(left, right, (((0,), (0,)), ((), ())), preferred_element_type=f32)
        out_ref[:, i * step : (i + 1) * step] = part.astype(bf16)


def small_call(body, out, *args, scalars=(), scratch=(), mib=8):
    smem = pl.BlockSpec(memory_space=pltpu.SMEM)
    vmem = pl.BlockSpec(memory_space=pltpu.VMEM)
    return pl.pallas_call(
        body,
        out_shape=out,
        in_specs=[smem] * len(scalars) + [vmem] * len(args),
        out_specs=vmem,
        scratch_shapes=list(scratch),
        compiler_params=pltpu.CompilerParams(vmem_limit_bytes=mib << 20),
        interpret=INTERPRET,
    )(*scalars, *args)


def swapped(v):
    return lax.ppermute(v, "c", [(0, 1), (1, 0)])


def weight_moves(ny, nx, nc):
    pairs = []
    for y in range(ny):
        for x in range(nx):
            for c in range(nc):
                upper = y // (ny // 2)
                at = (y * nx + x) * nc + c
                other = (((y + ny // 2) % ny) * nx + x) * nc + 1 - c
                pairs.append((at, at if upper == c else other))
    return pairs


def per_device(query, kv_pool, holder_table, slot_table, lengths, out_weight):
    ny, nx, nc = (lax.axis_size(a) for a in POOL)
    y, x, c = (lax.axis_index(a) for a in POOL)
    chips = ny * nx
    pos = jnp.stack([(y * nx + x) * nc + c, c]).astype(jnp.int32)

    kv_half = kv_pool.shape[-1] // nc
    kv_other = swapped(lax.dynamic_slice_in_dim(kv_pool, (1 - c) * kv_half, kv_half, axis=3))

    live = lax.broadcasted_iota(jnp.int32, holder_table.shape, 1) < lengths[:, None]
    table = jnp.concatenate([jnp.where(live, holder_table, -1), slot_table], axis=1).astype(bf16)
    width = HALF + table.shape[1]
    row = jnp.concatenate([query[:, :HALF], table, query[:, HALF:], table], axis=1).reshape(nc, 2, width // 2)
    rows = jnp.broadcast_to(row[None], (chips, nc, 2, width // 2)).reshape(chips * nc, 2, width // 2)
    q = lax.all_to_all(rows, POOL, split_axis=0, concat_axis=0, tiled=True).reshape(chips * nc, width)

    q, out_weight = lax.optimization_barrier((q, out_weight))
    weight = lax.ppermute(out_weight, POOL, weight_moves(ny, nx, nc))
    parts = attention_partials(pos, q, kv_pool, kv_other, chips)
    parts = lax.all_to_all(parts, CHIPS, split_axis=0, concat_axis=0, tiled=True)

    d_half = weight.shape[1] // nc
    w_got = swapped(lax.dynamic_slice_in_dim(weight, (1 - c) * d_half, d_half, axis=1))
    mine = small_call(merge_body, jax.ShapeDtypeStruct((64, chips * nc), bf16), parts,
                      scratch=[pltpu.VMEM((chips, chips * nc), f32)])
    got = swapped(mine)
    partial = small_call(
        project_body,
        jax.ShapeDtypeStruct((chips * nc, d_half), bf16),
        mine,
        got,
        weight,
        w_got,
        scalars=(pos,),
    )
    columns = lax.all_to_all(
        partial.reshape(chips, nc, d_half), CHIPS, split_axis=0, concat_axis=0, tiled=True
    )
    done = jnp.sum(columns.astype(f32), axis=0).astype(bf16)
    keep = lax.dynamic_slice_in_dim(done, c, 1, axis=0)
    got = swapped(lax.dynamic_slice_in_dim(done, 1 - c, 1, axis=0))
    return jnp.where(c == 0, jnp.concatenate([keep, got], axis=1), jnp.concatenate([got, keep], axis=1))


def solution(mesh):
    torus = Mesh(mesh.devices.reshape(mesh.shape["grp"], 8, 8, 2), GRP_POOL)
    return jax.shard_map(
        per_device,
        mesh=torus,
        in_specs=(
            P(GRP_POOL, None),
            P(GRP_POOL, None, None, None),
            P(GRP_POOL, None),
            P(GRP_POOL, None),
            P(GRP_POOL),
            P(POOL, None),
        ),
        out_specs=P(GRP_POOL, None),
        check_vma=False,
    )
```

```python
import functools
import math

import jax
import jax.numpy as jnp
from jax import lax
from jax.experimental import pallas as pl
from jax.experimental.pallas import tpu as pltpu
from jax.sharding import Mesh
from jax.sharding import PartitionSpec as P


H = 32
KVH = 4
HD = 128
GROUPS = H // KVH
CORES = 2
POOL = ("y", "x", "c")
CHIPS = ("y", "x")
GRP_POOL = ("grp", "y", "x", "c")
RATE = math.log2(math.e) / math.sqrt(HD)
TWICE = math.log(2.0) * math.sqrt(HD)
UNUSED = -32768.0
HALF = H * HD // CORES
INTERPRET = False

f32 = jnp.float32
bf16 = jnp.bfloat16


def as_product(value):
    pairs = []
    for i in range(128):
        mark = 1.0 + i / 128.0
        unit = 2.0 ** (math.floor(math.log2(value / mark)) - 7)
        bias = round(value / mark / unit) * unit
        pairs.append((abs(mark * bias - value), mark, bias))
    return min(pairs)[1:]


MARK, BIAS = as_product(TWICE)


def row_body(length_ref, q_ref, holder_ref, slot_ref, out_ref):
    devices, _, part = out_ref.shape
    lane = lax.broadcasted_iota(jnp.int32, holder_ref.shape, 1)
    holder = jnp.where(lane < length_ref[0], holder_ref[...], -1).astype(f32)
    table = [holder, slot_ref[...].astype(f32)]
    for core in range(CORES):
        row = jnp.concatenate([q_ref[:, core * HALF : (core + 1) * HALF].astype(f32)] + table, axis=1)
        row = jnp.concatenate([row[:, :part], row[:, part:]], axis=0).astype(bf16)

        def put(i, carry, row=row, core=core):
            out_ref[i * CORES + core] = row
            return carry

        lax.fori_loop(0, devices // CORES, put, 0)


def blocks_body(pos_ref, own_ref, other_ref, k_ref, v_ref):
    slots, _, blk, _ = own_ref.shape
    tokens = slots * blk
    token_slot = lax.broadcasted_iota(jnp.int32, (2 * tokens, HD), 0) // blk
    slot_lane = lax.broadcasted_iota(jnp.int32, (2 * tokens, HD), 1)
    mark = jnp.where(slot_lane == token_slot, MARK, 0.0).astype(bf16)
    for g in range(KVH // CORES):
        k_ref[g, :, HD:] = mark
        v_ref[g, HD:, :] = jnp.ones((v_ref.shape[1] - HD, 2 * tokens), bf16)
        at = pl.multiple_of((pos_ref[1] * (KVH // CORES) + g) * HD, HD)
        for i, (ref, cols) in enumerate(((own_ref, pl.ds(at, HD)), (other_ref, slice(g * HD, (g + 1) * HD)))):
            rows = slice(i * tokens, (i + 1) * tokens)
            k_ref[g, rows, :HD] = ref[:, 0, :, cols].reshape(tokens, HD)
            v_ref[g, :HD, rows] = ref[:, 1, :, cols].reshape(tokens, HD).T


def attention_body(pos_ref, q_ref, k_hbm, v_hbm, out_ref, k_ref, v_ref, s_scr, p_scr, sems):
    rows = q_ref.shape[0]
    steps, tokens, _ = k_ref.shape
    loads = {}
    for g in range(steps):
        for n, (source, target) in enumerate(((k_hbm, k_ref), (v_hbm, v_ref))):
            loads[n, g] = pltpu.make_async_copy(source.at[g], target.at[g], sems.at[n, g])
            loads[n, g].start()
    slots = HD // 2
    me, core = pos_ref[0], pos_ref[1]
    partner = me + 1 - 2 * core
    holder = q_ref[:, HALF : HALF + HD].astype(f32)
    slot = q_ref[:, HALF + HD : HALF + 2 * HD].astype(f32)
    lane = lax.broadcasted_iota(jnp.int32, (rows, HD), 1)
    lane_slot = jnp.where(lane < slots, lane, lane - slots).astype(f32)

    def bias_of(device):
        hit = holder == device.astype(f32)
        first = jnp.min(jnp.where(hit, slot, 999.0), axis=1, keepdims=True)
        last = jnp.max(jnp.where(hit, slot, -1.0), axis=1, keepdims=True)
        count = jnp.sum(jnp.where(hit, 1.0, 0.0), axis=1, keepdims=True)
        used = (lane_slot == first) | (lane_slot == last)
        double = used & (first == last) & (count > 1.5)
        return jnp.where(used, jnp.where(double, BIAS, 0.0), UNUSED)

    bias = jnp.where(lane < slots, bias_of(me), bias_of(partner)).astype(bf16)

    pairs = steps * GROUPS // 2
    chunk = 512
    chunks = tokens // chunk
    queries, peaks, outs = {}, {}, {}
    for i in range(pairs + 2):
        if i < pairs:
            heads = [q_ref[:, (2 * i + j) * HD : (2 * i + j + 1) * HD] for j in range(2)]
            queries[i] = jnp.concatenate([jnp.concatenate([q, bias], axis=1) for q in heads], axis=0)
            peaks[i] = None
            if 2 * i % GROUPS == 0:
                loads[0, 2 * i // GROUPS].wait()
        if 0 <= i - 2 and 2 * (i - 2) % GROUPS == 0:
            loads[1, 2 * (i - 2) // GROUPS].wait()
        if 0 <= i - 1 < pairs:
            top = jnp.max(peaks[i - 1], axis=0, keepdims=True).astype(bf16)
            peaks[i - 1] = top.astype(f32)
            for h in range(2):
                g, head = divmod(2 * (i - 1) + h, GROUPS)
                for j in range(4):
                    out_ref[dest_of(g, head, j), 32:33, :] = top[:, h * rows : (h + 1) * rows]
        for k in range(chunks):
            at = slice(k * chunk, (k + 1) * chunk)
            if i < pairs:
                s = lax.dot_general(
                    k_ref[2 * i // GROUPS, at, :], queries[i], (((1,), (1,)), ((), ())), preferred_element_type=f32
                )
                s_scr[i % 2, at, :] = s
                peak = jnp.max(s.reshape(chunk // 8, 8, 2 * rows), axis=0)
                peaks[i] = peak if peaks[i] is None else jnp.maximum(peaks[i], peak)
            if 0 <= i - 1 < pairs:
                n = i - 1
                p_scr[n % 2, at, :] = jnp.exp2((s_scr[n % 2, at, :] - peaks[n]) * RATE).astype(bf16)
            if 0 <= i - 2:
                n = i - 2
                out = jnp.dot(v_ref[2 * n // GROUPS, :, at], p_scr[n % 2, at, :], preferred_element_type=f32)
                outs[n] = out if k == 0 else outs[n] + out
        if 0 <= i - 2:
            out = outs.pop(i - 2)
            for h in range(2):
                g, head = divmod(2 * (i - 2) + h, GROUPS)
                cols = slice(h * rows, (h + 1) * rows)
                total = out[HD : HD + 1, cols]
                high = total.astype(bf16)
                low = (total - high.astype(f32)).astype(bf16)
                for j in range(4):
                    dest = dest_of(g, head, j)
                    out_ref[dest, 0:32, :] = out[j * 32 : (j + 1) * 32, cols].astype(bf16)
                    out_ref[dest, 33:34, :] = high
                    out_ref[dest, 34:35, :] = low


def dest_of(g, h, j):
    return ((j % 2) * 4 + g * 2 + h // 4) * 8 + (h % 4) * 2 + j // 2


def merge_body(got_ref, out_ref, f_scr):
    chips, _, rows = got_ref.shape
    peaks = [got_ref[i, 32:33, :].astype(f32) for i in range(chips)]
    top = functools.reduce(jnp.maximum, peaks)
    total = jnp.zeros((1, rows), f32)
    number = jnp.zeros((32, rows), f32)
    for i in range(chips):
        factor = jnp.exp2((peaks[i] - top) * RATE)
        total += factor * (got_ref[i, 33:34, :].astype(f32) + got_ref[i, 34:35, :].astype(f32))
        number += factor * got_ref[i, 0:32, :].astype(f32)
    attention = number / total
    high = attention.astype(bf16)
    out_ref[0:32, :] = high
    out_ref[32:64, :] = (attention - high.astype(f32)).astype(bf16)


def project_body(pos_ref, mine_ref, got_ref, w_ref, w_got_ref, out_ref):
    core = pos_ref[1]
    half = w_got_ref.shape[1]
    left = jnp.concatenate([mine_ref[...], got_ref[...]], axis=0)
    step = 512
    for i in range(half // step):
        cols = pl.ds(pl.multiple_of(core * half + i * step, step), step)
        mine = w_ref[:, cols]
        got = w_got_ref[:, i * step : (i + 1) * step]
        right = jnp.concatenate([mine, mine, got, got], axis=0)
        part = lax.dot_general(left, right, (((0,), (0,)), ((), ())), preferred_element_type=f32)
        out_ref[:, i * step : (i + 1) * step] = part.astype(bf16)


def small_call(body, out, *args, scalars=(), scratch=(), mib=8, flops=0, large=0):
    smem = pl.BlockSpec(memory_space=pltpu.SMEM)
    vmem = pl.BlockSpec(memory_space=pltpu.VMEM)
    return pl.pallas_call(
        body,
        out_shape=out,
        in_specs=[smem] * len(scalars) + [vmem] * (len(args) - large) + [pl.BlockSpec(memory_space=pltpu.HBM)] * large,
        out_specs=jax.tree.map(lambda _: vmem, out),
        scratch_shapes=list(scratch),
        cost_estimate=pl.CostEstimate(flops=flops, transcendentals=0, bytes_accessed=0) if flops else None,
        compiler_params=pltpu.CompilerParams(vmem_limit_bytes=mib << 20),
        interpret=INTERPRET,
    )(*scalars, *args)


def swapped(v):
    return lax.ppermute(v, "c", [(0, 1), (1, 0)])


def weight_moves(ny, nx, nc):
    pairs = []
    for y in range(ny):
        for x in range(nx):
            for c in range(nc):
                upper = y // (ny // 2)
                at = (y * nx + x) * nc + c
                other = (((y + ny // 2) % ny) * nx + x) * nc + 1 - c
                pairs.append((at, at if upper == c else other))
    return pairs


def per_device(query, kv_pool, holder_table, slot_table, lengths, out_weight):
    ny, nx, nc = (lax.axis_size(a) for a in POOL)
    y, x, c = (lax.axis_index(a) for a in POOL)
    chips = ny * nx
    pos = jnp.stack([(y * nx + x) * nc + c, c]).astype(jnp.int32)

    devices = chips * nc
    width = HALF + 2 * holder_table.shape[1]
    row_shape = jax.ShapeDtypeStruct((devices, 2, width // 2), bf16)
    rows = small_call(row_body, row_shape, query, holder_table, slot_table, scalars=(lengths,))
    q = lax.all_to_all(rows, POOL, split_axis=0, concat_axis=0, tiled=True)

    kv_half = kv_pool.shape[-1] // nc
    kv_other = swapped(lax.dynamic_slice_in_dim(kv_pool, (1 - c) * kv_half, kv_half, axis=3))
    tokens = nc * kv_pool.shape[0] * kv_pool.shape[2]
    steps = KVH // nc
    shapes = [jax.ShapeDtypeStruct((steps, tokens, 2 * HD), bf16), jax.ShapeDtypeStruct((steps, HD + 16, tokens), bf16)]
    keys, values = small_call(blocks_body, shapes, kv_pool, kv_other, scalars=(pos,), flops=1 << 32)

    q, out_weight = lax.optimization_barrier((q.reshape(devices, width), out_weight))
    weight = lax.ppermute(out_weight, POOL, weight_moves(ny, nx, nc))
    parts = small_call(
        attention_body,
        jax.ShapeDtypeStruct((chips, 40, devices), bf16),
        q,
        keys,
        values,
        scalars=(pos,),
        scratch=[
            *(pltpu.VMEM(v.shape, v.dtype) for v in shapes),
            pltpu.VMEM((2, tokens, 2 * devices), f32),
            pltpu.VMEM((2, tokens, 2 * devices), bf16),
            pltpu.SemaphoreType.DMA((2, steps)),
        ],
        mib=62,
        large=2,
        flops=1 << 34,
    )
    parts = lax.all_to_all(parts, CHIPS, split_axis=0, concat_axis=0, tiled=True)

    d_half = weight.shape[1] // nc
    w_got = swapped(lax.dynamic_slice_in_dim(weight, (1 - c) * d_half, d_half, axis=1))
    mine = small_call(merge_body, jax.ShapeDtypeStruct((64, chips * nc), bf16), parts,
                      scratch=[pltpu.VMEM((chips, chips * nc), f32)])
    got = swapped(mine)
    partial = small_call(
        project_body,
        jax.ShapeDtypeStruct((chips * nc, d_half), bf16),
        mine,
        got,
        weight,
        w_got,
        scalars=(pos,),
    )
    columns = lax.all_to_all(
        partial.reshape(chips, nc, d_half), CHIPS, split_axis=0, concat_axis=0, tiled=True
    )
    done = jnp.sum(columns.astype(f32), axis=0).astype(bf16)
    keep = lax.dynamic_slice_in_dim(done, c, 1, axis=0)
    got = swapped(lax.dynamic_slice_in_dim(done, 1 - c, 1, axis=0))
    return jnp.where(c == 0, jnp.concatenate([keep, got], axis=1), jnp.concatenate([got, keep], axis=1))


def solution(mesh):
    torus = Mesh(mesh.devices.reshape(mesh.shape["grp"], 8, 8, 2), GRP_POOL)
    return jax.shard_map(
        per_device,
        mesh=torus,
        in_specs=(
            P(GRP_POOL, None),
            P(GRP_POOL, None, None, None),
            P(GRP_POOL, None),
            P(GRP_POOL, None),
            P(GRP_POOL),
            P(POOL, None),
        ),
        out_specs=P(GRP_POOL, None),
        check_vma=False,
    )
```

```python
import functools
import math

import jax
import jax.numpy as jnp
from jax import lax
from jax.experimental import pallas as pl
from jax.experimental.pallas import tpu as pltpu
from jax.sharding import Mesh
from jax.sharding import PartitionSpec as P


H = 32
KVH = 4
HD = 128
GROUPS = H // KVH
CORES = 2
POOL = ("y", "x", "c")
CHIPS = ("y", "x")
GRP_POOL = ("grp", "y", "x", "c")
RATE = math.log2(math.e) / math.sqrt(HD)
TWICE = math.log(2.0) * math.sqrt(HD)
UNUSED = -32768.0
HALF = H * HD // CORES
TILE = 2 * HD
VROWS = HD + 16
INTERPRET = False

f32 = jnp.float32
bf16 = jnp.bfloat16


def as_product(value):
    pairs = []
    for i in range(128):
        mark = 1.0 + i / 128.0
        unit = 2.0 ** (math.floor(math.log2(value / mark)) - 7)
        bias = round(value / mark / unit) * unit
        pairs.append((abs(mark * bias - value), mark, bias))
    return min(pairs)[1:]


MARK, BIAS = as_product(TWICE)


def row_body(length_ref, q_ref, holder_ref, slot_ref, out_ref):
    devices, _, part = out_ref.shape
    lane = lax.broadcasted_iota(jnp.int32, holder_ref.shape, 1)
    holder = jnp.where(lane < length_ref[0], holder_ref[...], -1).astype(f32)
    table = [holder, slot_ref[...].astype(f32)]
    for core in range(CORES):
        row = jnp.concatenate([q_ref[:, core * HALF : (core + 1) * HALF].astype(f32)] + table, axis=1)
        row = jnp.concatenate([row[:, :part], row[:, part:]], axis=0).astype(bf16)

        def put(i, carry, row=row, core=core):
            out_ref[i * CORES + core] = row
            return carry

        lax.fori_loop(0, devices // CORES, put, 0)


def blocks_body(pos_ref, own_ref, other_ref, out_ref):
    slots, _, blk, _ = own_ref.shape
    tokens = slots * blk
    token_slot = lax.broadcasted_iota(jnp.int32, (2 * tokens, HD), 0) // blk
    slot_lane = lax.broadcasted_iota(jnp.int32, (2 * tokens, HD), 1)
    mark = jnp.where(slot_lane == token_slot, MARK, 0.0).astype(bf16)
    for g in range(KVH // CORES):
        out_ref[g, : 2 * tokens, HD:] = mark
        at = pl.ds(pl.multiple_of((pos_ref[1] * (KVH // CORES) + g) * HD, HD), HD)
        for i, ref in enumerate((own_ref, other_ref)):
            out_ref[g, i * tokens : (i + 1) * tokens, :HD] = ref[:, 0, :, at].reshape(tokens, HD)
            turned = ref[:, 1, :, at].reshape(tokens, HD).T
            for j in range(tokens // TILE):
                row = 2 * tokens + (i * (tokens // TILE) + j) * VROWS
                out_ref[g, row : row + HD, :] = turned[:, j * TILE : (j + 1) * TILE]
                out_ref[g, row + HD : row + VROWS, :] = jnp.ones((VROWS - HD, TILE), bf16)


def attention_body(pos_ref, q_ref, kv_hbm, out_ref, kv_ref, s_scr, p_scr, sems):
    rows = q_ref.shape[0]
    steps = kv_ref.shape[0]
    tokens = s_scr.shape[1]
    loads = {}
    for g in range(steps):
        for n, at in enumerate((slice(0, tokens), slice(tokens, kv_ref.shape[1]))):
            loads[n, g] = pltpu.make_async_copy(kv_hbm.at[g, at], kv_ref.at[g, at], sems.at[n, g])
            loads[n, g].start()
    slots = HD // 2
    me, core = pos_ref[0], pos_ref[1]
    partner = me + 1 - 2 * core
    holder = q_ref[:, HALF : HALF + HD].astype(f32)
    slot = q_ref[:, HALF + HD : HALF + 2 * HD].astype(f32)
    lane = lax.broadcasted_iota(jnp.int32, (rows, HD), 1)
    lane_slot = jnp.where(lane < slots, lane, lane - slots).astype(f32)

    def bias_of(device):
        hit = holder == device.astype(f32)
        first = jnp.min(jnp.where(hit, slot, 999.0), axis=1, keepdims=True)
        last = jnp.max(jnp.where(hit, slot, -1.0), axis=1, keepdims=True)
        count = jnp.sum(jnp.where(hit, 1.0, 0.0), axis=1, keepdims=True)
        used = (lane_slot == first) | (lane_slot == last)
        double = used & (first == last) & (count > 1.5)
        return jnp.where(used, jnp.where(double, BIAS, 0.0), UNUSED)

    bias = jnp.where(lane < slots, bias_of(me), bias_of(partner)).astype(bf16)

    pairs = steps * GROUPS // 2
    chunk = 512
    chunks = tokens // chunk
    queries, peaks, outs = {}, {}, {}
    for i in range(pairs + 2):
        if i < pairs:
            heads = [q_ref[:, (2 * i + j) * HD : (2 * i + j + 1) * HD] for j in range(2)]
            queries[i] = jnp.concatenate([jnp.concatenate([q, bias], axis=1) for q in heads], axis=0)
            peaks[i] = None
            if 2 * i % GROUPS == 0:
                loads[0, 2 * i // GROUPS].wait()
        if 0 <= i - 2 and 2 * (i - 2) % GROUPS == 0:
            loads[1, 2 * (i - 2) // GROUPS].wait()
        if 0 <= i - 1 < pairs:
            top = jnp.max(peaks[i - 1], axis=0, keepdims=True).astype(bf16)
            peaks[i - 1] = top.astype(f32)
            for h in range(2):
                g, head = divmod(2 * (i - 1) + h, GROUPS)
                for j in range(4):
                    out_ref[dest_of(g, head, j), 32:33, :] = top[:, h * rows : (h + 1) * rows]
        for k in range(chunks):
            at = slice(k * chunk, (k + 1) * chunk)
            if i < pairs:
                s = lax.dot_general(
                    kv_ref[2 * i // GROUPS, at, :], queries[i], (((1,), (1,)), ((), ())), preferred_element_type=f32
                )
                s_scr[i % 2, at, :] = s
                peak = jnp.max(s.reshape(chunk // 8, 8, 2 * rows), axis=0)
                peaks[i] = peak if peaks[i] is None else jnp.maximum(peaks[i], peak)
            if 0 <= i - 1 < pairs:
                n = i - 1
                p_scr[n % 2, at, :] = jnp.exp2((s_scr[n % 2, at, :] - peaks[n]) * RATE).astype(bf16)
            if 0 <= i - 2:
                n = i - 2
                tiles = [
                    kv_ref[2 * n // GROUPS, tokens + j * VROWS : tokens + (j + 1) * VROWS, :]
                    for j in range(k * chunk // TILE, (k + 1) * chunk // TILE)
                ]
                out = jnp.dot(jnp.concatenate(tiles, axis=1), p_scr[n % 2, at, :], preferred_element_type=f32)
                outs[n] = out if k == 0 else outs[n] + out
        if 0 <= i - 2:
            out = outs.pop(i - 2)
            for h in range(2):
                g, head = divmod(2 * (i - 2) + h, GROUPS)
                cols = slice(h * rows, (h + 1) * rows)
                total = out[HD : HD + 1, cols]
                high = total.astype(bf16)
                low = (total - high.astype(f32)).astype(bf16)
                for j in range(4):
                    dest = dest_of(g, head, j)
                    out_ref[dest, 0:32, :] = out[j * 32 : (j + 1) * 32, cols].astype(bf16)
                    out_ref[dest, 33:34, :] = high
                    out_ref[dest, 34:35, :] = low


def dest_of(g, h, j):
    return ((j % 2) * 4 + g * 2 + h // 4) * 8 + (h % 4) * 2 + j // 2


def merge_body(got_ref, out_ref):
    chips, _, rows = got_ref.shape
    peaks = [got_ref[i, 32:33, :].astype(f32) for i in range(chips)]
    top = functools.reduce(jnp.maximum, peaks)
    total = jnp.zeros((1, rows), f32)
    number = jnp.zeros((32, rows), f32)
    for i in range(chips):
        factor = jnp.exp2((peaks[i] - top) * RATE)
        total += factor * (got_ref[i, 33:34, :].astype(f32) + got_ref[i, 34:35, :].astype(f32))
        number += factor * got_ref[i, 0:32, :].astype(f32)
    attention = number / total
    high = attention.astype(bf16)
    out_ref[0:32, :] = high
    out_ref[32:64, :] = (attention - high.astype(f32)).astype(bf16)


def project_body(*refs):
    count = len(refs) // 2
    lefts, rights, out_ref = refs[:count], refs[count:-1], refs[-1]
    left = jnp.concatenate([r[...] for r in lefts], axis=0)
    step = 512
    for i in range(out_ref.shape[1] // step):
        cols = slice(i * step, (i + 1) * step)
        right = jnp.concatenate([r[:, cols] for r in rights for _ in range(2)], axis=0)
        part = lax.dot_general(left, right, (((0,), (0,)), ((), ())), preferred_element_type=f32)
        out_ref[:, cols] = part.astype(bf16)


def small_call(body, out, *args, scalars=(), scratch=(), mib=8, flops=0, large=0):
    smem = pl.BlockSpec(memory_space=pltpu.SMEM)
    vmem = pl.BlockSpec(memory_space=pltpu.VMEM)
    return pl.pallas_call(
        body,
        out_shape=out,
        in_specs=[smem] * len(scalars) + [vmem] * (len(args) - large) + [pl.BlockSpec(memory_space=pltpu.HBM)] * large,
        out_specs=jax.tree.map(lambda _: vmem, out),
        scratch_shapes=list(scratch),
        cost_estimate=pl.CostEstimate(flops=flops, transcendentals=0, bytes_accessed=0) if flops else None,
        compiler_params=pltpu.CompilerParams(vmem_limit_bytes=mib << 20),
        interpret=INTERPRET,
    )(*scalars, *args)


def swapped(v):
    return lax.ppermute(v, "c", [(0, 1), (1, 0)])


def to_mate(v, k):
    nx, nc = lax.axis_size("x"), lax.axis_size("c")
    perm = [(x * nc + c, (x ^ (k // nc)) * nc + (c ^ (k % nc))) for x in range(nx) for c in range(nc)]
    return lax.ppermute(v, ("x", "c"), perm)


def weight_moves(ny, nx, nc):
    pairs = []
    for y in range(ny):
        for x in range(nx):
            for c in range(nc):
                upper = y // (ny // 2)
                at = (y * nx + x) * nc + c
                other = (((y + ny // 2) % ny) * nx + x) * nc + 1 - c
                pairs.append((at, at if upper == c else other))
    return pairs


def per_device(query, kv_pool, holder_table, slot_table, lengths, out_weight):
    ny, nx, nc = (lax.axis_size(a) for a in POOL)
    y, x, c = (lax.axis_index(a) for a in POOL)
    chips = ny * nx
    pos = jnp.stack([(y * nx + x) * nc + c, c]).astype(jnp.int32)

    devices = chips * nc
    width = HALF + 2 * holder_table.shape[1]
    row_shape = jax.ShapeDtypeStruct((devices, 2, width // 2), bf16)
    rows = small_call(row_body, row_shape, query, holder_table, slot_table, scalars=(lengths,))
    weight = lax.ppermute(out_weight, POOL, weight_moves(ny, nx, nc))
    q = lax.all_to_all(rows, POOL, split_axis=0, concat_axis=0, tiled=True)

    kv_other = swapped(kv_pool)
    tokens = nc * kv_pool.shape[0] * kv_pool.shape[2]
    steps = KVH // nc
    kv_shape = (steps, tokens + tokens // TILE * VROWS, TILE)
    blocks = small_call(
        blocks_body, jax.ShapeDtypeStruct(kv_shape, bf16), kv_pool, kv_other, scalars=(pos,), flops=1 << 32
    )

    mates = 2 * nc
    mate = (x % 2) * nc + c
    d_part = weight.shape[1] // mates
    weights = []
    for k in range(mates):
        part = lax.dynamic_slice_in_dim(weight, (mate ^ k) * d_part, d_part, axis=1)
        weights.append(to_mate(part, k) if k else part)

    q, *weights = lax.optimization_barrier((q.reshape(devices, width), *weights))
    parts = small_call(
        attention_body,
        jax.ShapeDtypeStruct((chips, 40, devices), bf16),
        q,
        blocks,
        scalars=(pos,),
        scratch=[
            pltpu.VMEM(kv_shape, bf16),
            pltpu.VMEM((2, tokens, 2 * devices), f32),
            pltpu.VMEM((2, tokens, 2 * devices), bf16),
            pltpu.SemaphoreType.DMA((2, steps)),
        ],
        mib=52,
        large=1,
        flops=1 << 34,
    )
    parts = lax.all_to_all(parts, CHIPS, split_axis=0, concat_axis=0, tiled=True)
    mine = small_call(merge_body, jax.ShapeDtypeStruct((64, devices), bf16), parts)
    lefts = [to_mate(mine, k) if k else mine for k in range(mates)]
    partial = small_call(project_body, jax.ShapeDtypeStruct((devices, d_part), bf16), *lefts, *weights)
    columns = lax.all_to_all(
        partial.reshape(devices, 2, d_part // 2), POOL, split_axis=0, concat_axis=0, tiled=True
    )
    done = jnp.sum(columns.reshape(devices // mates, mates, d_part).astype(f32), axis=0).astype(bf16)
    return done.reshape(1, mates * d_part)


def solution(mesh):
    torus = Mesh(mesh.devices.reshape(mesh.shape["grp"], 8, 8, 2), GRP_POOL)
    return jax.shard_map(
        per_device,
        mesh=torus,
        in_specs=(
            P(GRP_POOL, None),
            P(GRP_POOL, None, None, None),
            P(GRP_POOL, None),
            P(GRP_POOL, None),
            P(GRP_POOL),
            P(POOL, None),
        ),
        out_specs=P(GRP_POOL, None),
        check_vma=False,
    )
```

```python
import functools
import math

import jax
import jax.numpy as jnp
from jax import lax
from jax.experimental import pallas as pl
from jax.experimental.pallas import tpu as pltpu
from jax.sharding import Mesh
from jax.sharding import PartitionSpec as P


H = 32
KVH = 4
HD = 128
GROUPS = H // KVH
CORES = 2
POOL = ("y", "x", "c")
CHIPS = ("y", "x")
GRP_POOL = ("grp", "y", "x", "c")
RATE = math.log2(math.e) / math.sqrt(HD)
TWICE = math.log(2.0) * math.sqrt(HD)
UNUSED = -32768.0
HALF = H * HD // CORES
TILE = 2 * HD
VROWS = HD + 16
INTERPRET = False

f32 = jnp.float32
bf16 = jnp.bfloat16


def as_product(value):
    pairs = []
    for i in range(128):
        mark = 1.0 + i / 128.0
        unit = 2.0 ** (math.floor(math.log2(value / mark)) - 7)
        bias = round(value / mark / unit) * unit
        pairs.append((abs(mark * bias - value), mark, bias))
    return min(pairs)[1:]


MARK, BIAS = as_product(TWICE)


def row_body(length_ref, q_hbm, holder_hbm, slot_hbm, out_ref, q_ref, holder_ref, slot_ref, sems):
    pairs = ((q_hbm, q_ref), (holder_hbm, holder_ref), (slot_hbm, slot_ref))
    loads = [pltpu.make_async_copy(source, target, sems.at[n]) for n, (source, target) in enumerate(pairs)]
    for load in loads:
        load.start()
    for load in loads:
        load.wait()
    devices, _, part = out_ref.shape
    lane = lax.broadcasted_iota(jnp.int32, holder_ref.shape, 1)
    holder = jnp.where(lane < length_ref[0], holder_ref[...], -1).astype(f32)
    table = [holder, slot_ref[...].astype(f32)]
    for core in range(CORES):
        row = jnp.concatenate([q_ref[:, core * HALF : (core + 1) * HALF].astype(f32)] + table, axis=1)
        row = jnp.concatenate([row[:, :part], row[:, part:]], axis=0).astype(bf16)

        def put(i, carry, row=row, core=core):
            out_ref[i * CORES + core] = row
            return carry

        lax.fori_loop(0, devices // CORES, put, 0)


def blocks_body(pos_ref, own_ref, other_ref, out_ref):
    slots, _, blk, _ = own_ref.shape
    tokens = slots * blk
    token_slot = lax.broadcasted_iota(jnp.int32, (2 * tokens, HD), 0) // blk
    slot_lane = lax.broadcasted_iota(jnp.int32, (2 * tokens, HD), 1)
    mark = jnp.where(slot_lane == token_slot, MARK, 0.0).astype(bf16)
    for g in range(KVH // CORES):
        out_ref[g, : 2 * tokens, HD:] = mark
        at = pl.ds(pl.multiple_of((pos_ref[1] * (KVH // CORES) + g) * HD, HD), HD)
        for i, ref in enumerate((own_ref, other_ref)):
            out_ref[g, i * tokens : (i + 1) * tokens, :HD] = ref[:, 0, :, at].reshape(tokens, HD)
            turned = ref[:, 1, :, at].reshape(tokens, HD).T
            for j in range(tokens // TILE):
                row = 2 * tokens + (i * (tokens // TILE) + j) * VROWS
                out_ref[g, row : row + HD, :] = turned[:, j * TILE : (j + 1) * TILE]
                out_ref[g, row + HD : row + VROWS, :] = jnp.ones((VROWS - HD, TILE), bf16)


def attention_body(pos_ref, q_ref, kv_hbm, out_ref, kv_ref, s_scr, p_scr, sems):
    rows = q_ref.shape[0]
    steps = kv_ref.shape[0]
    tokens = s_scr.shape[1]
    loads = {}
    for g in range(steps):
        for n, at in enumerate((slice(0, tokens), slice(tokens, kv_ref.shape[1]))):
            loads[n, g] = pltpu.make_async_copy(kv_hbm.at[g, at], kv_ref.at[g, at], sems.at[n, g])
            loads[n, g].start()
    slots = HD // 2
    me, core = pos_ref[0], pos_ref[1]
    partner = me + 1 - 2 * core
    holder = q_ref[:, HALF : HALF + HD].astype(f32)
    slot = q_ref[:, HALF + HD : HALF + 2 * HD].astype(f32)
    lane = lax.broadcasted_iota(jnp.int32, (rows, HD), 1)
    lane_slot = jnp.where(lane < slots, lane, lane - slots).astype(f32)

    def bias_of(device):
        hit = holder == device.astype(f32)
        first = jnp.min(jnp.where(hit, slot, 999.0), axis=1, keepdims=True)
        last = jnp.max(jnp.where(hit, slot, -1.0), axis=1, keepdims=True)
        count = jnp.sum(jnp.where(hit, 1.0, 0.0), axis=1, keepdims=True)
        used = (lane_slot == first) | (lane_slot == last)
        double = used & (first == last) & (count > 1.5)
        return jnp.where(used, jnp.where(double, BIAS, 0.0), UNUSED)

    bias = jnp.where(lane < slots, bias_of(me), bias_of(partner)).astype(bf16)

    pairs = steps * GROUPS // 2
    chunk = 512
    chunks = tokens // chunk
    queries, peaks, outs = {}, {}, {}
    for i in range(pairs + 2):
        if i < pairs:
            heads = [q_ref[:, (2 * i + j) * HD : (2 * i + j + 1) * HD] for j in range(2)]
            queries[i] = jnp.concatenate([jnp.concatenate([q, bias], axis=1) for q in heads], axis=0)
            peaks[i] = None
            if 2 * i % GROUPS == 0:
                loads[0, 2 * i // GROUPS].wait()
        if 0 <= i - 2 and 2 * (i - 2) % GROUPS == 0:
            loads[1, 2 * (i - 2) // GROUPS].wait()
        if 0 <= i - 1 < pairs:
            top = jnp.max(peaks[i - 1], axis=0, keepdims=True).astype(bf16)
            peaks[i - 1] = top.astype(f32)
            for h in range(2):
                g, head = divmod(2 * (i - 1) + h, GROUPS)
                for j in range(4):
                    out_ref[dest_of(g, head, j), 32:33, :] = top[:, h * rows : (h + 1) * rows]
        for k in range(chunks):
            at = slice(k * chunk, (k + 1) * chunk)
            if i < pairs:
                s = lax.dot_general(
                    kv_ref[2 * i // GROUPS, at, :], queries[i], (((1,), (1,)), ((), ())), preferred_element_type=f32
                )
                s_scr[i % 2, at, :] = s
                peak = jnp.max(s.reshape(chunk // 8, 8, 2 * rows), axis=0)
                peaks[i] = peak if peaks[i] is None else jnp.maximum(peaks[i], peak)
            if 0 <= i - 1 < pairs:
                n = i - 1
                p_scr[n % 2, at, :] = jnp.exp2((s_scr[n % 2, at, :] - peaks[n]) * RATE).astype(bf16)
            if 0 <= i - 2:
                n = i - 2
                tiles = [
                    kv_ref[2 * n // GROUPS, tokens + j * VROWS : tokens + (j + 1) * VROWS, :]
                    for j in range(k * chunk // TILE, (k + 1) * chunk // TILE)
                ]
                out = jnp.dot(jnp.concatenate(tiles, axis=1), p_scr[n % 2, at, :], preferred_element_type=f32)
                outs[n] = out if k == 0 else outs[n] + out
        if 0 <= i - 2:
            out = outs.pop(i - 2)
            for h in range(2):
                g, head = divmod(2 * (i - 2) + h, GROUPS)
                cols = slice(h * rows, (h + 1) * rows)
                total = out[HD : HD + 1, cols]
                high = total.astype(bf16)
                low = (total - high.astype(f32)).astype(bf16)
                for j in range(4):
                    dest = dest_of(g, head, j)
                    out_ref[dest, 0:32, :] = out[j * 32 : (j + 1) * 32, cols].astype(bf16)
                    out_ref[dest, 33:34, :] = high
                    out_ref[dest, 34:35, :] = low


def dest_of(g, h, j):
    return ((j % 2) * 4 + g * 2 + h // 4) * 8 + (h % 4) * 2 + j // 2


def merge_body(got_ref, out_ref):
    chips, _, rows = got_ref.shape
    peaks = [got_ref[i, 32:33, :].astype(f32) for i in range(chips)]
    top = functools.reduce(jnp.maximum, peaks)
    total = jnp.zeros((1, rows), f32)
    number = jnp.zeros((32, rows), f32)
    for i in range(chips):
        factor = jnp.exp2((peaks[i] - top) * RATE)
        total += factor * (got_ref[i, 33:34, :].astype(f32) + got_ref[i, 34:35, :].astype(f32))
        number += factor * got_ref[i, 0:32, :].astype(f32)
    attention = number / total
    high = attention.astype(bf16)
    out_ref[0:32, :] = high
    out_ref[32:64, :] = (attention - high.astype(f32)).astype(bf16)


def project_body(*refs):
    count = len(refs) // 2
    lefts, rights, out_ref = refs[:count], refs[count:-1], refs[-1]
    left = jnp.concatenate([r[...] for r in lefts], axis=0)
    step = 512
    for i in range(out_ref.shape[1] // step):
        cols = slice(i * step, (i + 1) * step)
        right = jnp.concatenate([r[:, cols] for r in rights for _ in range(2)], axis=0)
        part = lax.dot_general(left, right, (((0,), (0,)), ((), ())), preferred_element_type=f32)
        out_ref[:, cols] = part.astype(bf16)


def finish_body(got_ref, out_ref):
    devices, parts, part = got_ref.shape
    mates = out_ref.shape[1] // (parts * part)
    for m in range(mates):
        total = sum(got_ref[i].astype(f32) for i in range(m, devices, mates)).astype(bf16)
        for r in range(parts):
            at = (m * parts + r) * part
            out_ref[:, at : at + part] = total[r : r + 1]


def small_call(body, out, *args, scalars=(), scratch=(), mib=8, flops=0, large=0):
    smem = pl.BlockSpec(memory_space=pltpu.SMEM)
    vmem = pl.BlockSpec(memory_space=pltpu.VMEM)
    return pl.pallas_call(
        body,
        out_shape=out,
        in_specs=[smem] * len(scalars) + [vmem] * (len(args) - large) + [pl.BlockSpec(memory_space=pltpu.HBM)] * large,
        out_specs=jax.tree.map(lambda _: vmem, out),
        scratch_shapes=list(scratch),
        cost_estimate=pl.CostEstimate(flops=flops, transcendentals=0, bytes_accessed=0) if flops else None,
        compiler_params=pltpu.CompilerParams(vmem_limit_bytes=mib << 20),
        interpret=INTERPRET,
    )(*scalars, *args)


def swapped(v):
    return lax.ppermute(v, "c", [(0, 1), (1, 0)])


def to_mate(v, k):
    nx, nc = lax.axis_size("x"), lax.axis_size("c")
    perm = [(x * nc + c, (x ^ (k // nc)) * nc + (c ^ (k % nc))) for x in range(nx) for c in range(nc)]
    return lax.ppermute(v, ("x", "c"), perm)


def weight_moves(ny, nx, nc):
    pairs = []
    for y in range(ny):
        for x in range(nx):
            for c in range(nc):
                upper = y // (ny // 2)
                at = (y * nx + x) * nc + c
                other = (((y + ny // 2) % ny) * nx + x) * nc + 1 - c
                pairs.append((at, at if upper == c else other))
    return pairs


def per_device(query, kv_pool, holder_table, slot_table, lengths, out_weight):
    ny, nx, nc = (lax.axis_size(a) for a in POOL)
    y, x, c = (lax.axis_index(a) for a in POOL)
    chips = ny * nx
    pos = jnp.stack([(y * nx + x) * nc + c, c]).astype(jnp.int32)

    devices = chips * nc
    width = HALF + 2 * holder_table.shape[1]
    row_shape = jax.ShapeDtypeStruct((devices, 2, width // 2), bf16)
    scratch = [pltpu.VMEM(v.shape, v.dtype) for v in (query, holder_table, slot_table)]
    rows = small_call(
        row_body,
        row_shape,
        query,
        holder_table,
        slot_table,
        scalars=(lengths,),
        scratch=[*scratch, pltpu.SemaphoreType.DMA((3,))],
        large=3,
        mib=62,
    )
    weight = lax.ppermute(out_weight, POOL, weight_moves(ny, nx, nc))
    q = lax.all_to_all(rows, POOL, split_axis=0, concat_axis=0, tiled=True)

    kv_other = swapped(kv_pool)
    tokens = nc * kv_pool.shape[0] * kv_pool.shape[2]
    steps = KVH // nc
    kv_shape = (steps, tokens + tokens // TILE * VROWS, TILE)
    blocks = small_call(
        blocks_body, jax.ShapeDtypeStruct(kv_shape, bf16), kv_pool, kv_other, scalars=(pos,), flops=1 << 32
    )

    mates = 2 * nc
    mate = (x % 2) * nc + c
    d_part = weight.shape[1] // mates
    weights = []
    for k in range(mates):
        part = lax.dynamic_slice_in_dim(weight, (mate ^ k) * d_part, d_part, axis=1)
        weights.append(to_mate(part, k) if k else part)

    q = q.reshape(devices, width)
    parts = small_call(
        attention_body,
        jax.ShapeDtypeStruct((chips, 40, devices), bf16),
        q,
        blocks,
        scalars=(pos,),
        scratch=[
            pltpu.VMEM(kv_shape, bf16),
            pltpu.VMEM((2, tokens, 2 * devices), f32),
            pltpu.VMEM((2, tokens, 2 * devices), bf16),
            pltpu.SemaphoreType.DMA((2, steps)),
        ],
        mib=52,
        large=1,
        flops=1 << 34,
    )
    parts = lax.all_to_all(parts, CHIPS, split_axis=0, concat_axis=0, tiled=True)
    mine = small_call(merge_body, jax.ShapeDtypeStruct((64, devices), bf16), parts)
    lefts = [to_mate(mine, k) if k else mine for k in range(mates)]
    partial = small_call(project_body, jax.ShapeDtypeStruct((devices, d_part), bf16), *lefts, *weights)
    columns = lax.all_to_all(
        partial.reshape(devices, 2, d_part // 2), POOL, split_axis=0, concat_axis=0, tiled=True
    )
    return small_call(finish_body, jax.ShapeDtypeStruct((1, mates * d_part), bf16), columns)


def solution(mesh):
    torus = Mesh(mesh.devices.reshape(mesh.shape["grp"], 8, 8, 2), GRP_POOL)
    return jax.shard_map(
        per_device,
        mesh=torus,
        in_specs=(
            P(GRP_POOL, None),
            P(GRP_POOL, None, None, None),
            P(GRP_POOL, None),
            P(GRP_POOL, None),
            P(GRP_POOL),
            P(POOL, None),
        ),
        out_specs=P(GRP_POOL, None),
        check_vma=False,
    )
```

```python
import functools
import math

import jax
import jax.numpy as jnp
from jax import lax
from jax.experimental import pallas as pl
from jax.experimental.pallas import tpu as pltpu
from jax.sharding import Mesh
from jax.sharding import PartitionSpec as P


H = 32
KVH = 4
HD = 128
GROUPS = H // KVH
CORES = 2
POOL = ("y", "x", "c")
CHIPS = ("y", "x")
GRP_POOL = ("grp", "y", "x", "c")
RATE = math.log2(math.e) / math.sqrt(HD)
TWICE = math.log(2.0) * math.sqrt(HD)
UNUSED = -32768.0
HALF = H * HD // CORES
TILE = 2 * HD
VROWS = HD + 16
INTERPRET = False

f32 = jnp.float32
bf16 = jnp.bfloat16


def as_product(value):
    pairs = []
    for i in range(128):
        mark = 1.0 + i / 128.0
        unit = 2.0 ** (math.floor(math.log2(value / mark)) - 7)
        bias = round(value / mark / unit) * unit
        pairs.append((abs(mark * bias - value), mark, bias))
    return min(pairs)[1:]


MARK, BIAS = as_product(TWICE)


def row_body(length_ref, q_hbm, holder_hbm, slot_hbm, out_ref, q_ref, holder_ref, slot_ref, sems):
    pairs = ((q_hbm, q_ref), (holder_hbm, holder_ref), (slot_hbm, slot_ref))
    loads = [pltpu.make_async_copy(source, target, sems.at[n]) for n, (source, target) in enumerate(pairs)]
    for load in loads:
        load.start()
    for load in loads:
        load.wait()
    devices, _, part = out_ref.shape
    lane = lax.broadcasted_iota(jnp.int32, holder_ref.shape, 1)
    holder = jnp.where(lane < length_ref[0], holder_ref[...], -1).astype(f32)
    table = [holder, slot_ref[...].astype(f32)]
    for core in range(CORES):
        row = jnp.concatenate([q_ref[:, core * HALF : (core + 1) * HALF].astype(f32)] + table, axis=1)
        row = jnp.concatenate([row[:, :part], row[:, part:]], axis=0).astype(bf16)

        def put(i, carry, row=row, core=core):
            out_ref[i * CORES + core] = row
            return carry

        lax.fori_loop(0, devices // CORES, put, 0)


def blocks_body(pos_ref, own_ref, other_ref, out_ref):
    slots, _, blk, _ = own_ref.shape
    tokens = slots * blk
    token_slot = lax.broadcasted_iota(jnp.int32, (2 * tokens, HD), 0) // blk
    slot_lane = lax.broadcasted_iota(jnp.int32, (2 * tokens, HD), 1)
    mark = jnp.where(slot_lane == token_slot, MARK, 0.0).astype(bf16)
    for g in range(KVH // CORES):
        out_ref[g, : 2 * tokens, HD:] = mark
        at = pl.ds(pl.multiple_of((pos_ref[1] * (KVH // CORES) + g) * HD, HD), HD)
        for i, ref in enumerate((own_ref, other_ref)):
            out_ref[g, i * tokens : (i + 1) * tokens, :HD] = ref[:, 0, :, at].reshape(tokens, HD)
            turned = ref[:, 1, :, at].reshape(tokens, HD).T
            for j in range(tokens // TILE):
                row = 2 * tokens + (i * (tokens // TILE) + j) * VROWS
                out_ref[g, row : row + HD, :] = turned[:, j * TILE : (j + 1) * TILE]
                out_ref[g, row + HD : row + VROWS, :] = jnp.ones((VROWS - HD, TILE), bf16)


def attention_body(pos_ref, q_ref, kv_hbm, out_ref, kv_ref, s_scr, p_scr, sems):
    rows = q_ref.shape[0]
    steps = kv_ref.shape[0]
    tokens = s_scr.shape[1]
    loads = {}
    for g in range(steps):
        for n, at in enumerate((slice(0, tokens), slice(tokens, kv_ref.shape[1]))):
            loads[n, g] = pltpu.make_async_copy(kv_hbm.at[g, at], kv_ref.at[g, at], sems.at[n, g])
            loads[n, g].start()
    slots = HD // 2
    me, core = pos_ref[0], pos_ref[1]
    partner = me + 1 - 2 * core
    holder = q_ref[:, HALF : HALF + HD].astype(f32)
    slot = q_ref[:, HALF + HD : HALF + 2 * HD].astype(f32)
    lane = lax.broadcasted_iota(jnp.int32, (rows, HD), 1)
    lane_slot = jnp.where(lane < slots, lane, lane - slots).astype(f32)

    def bias_of(device):
        hit = holder == device.astype(f32)
        first = jnp.min(jnp.where(hit, slot, 999.0), axis=1, keepdims=True)
        last = jnp.max(jnp.where(hit, slot, -1.0), axis=1, keepdims=True)
        count = jnp.sum(jnp.where(hit, 1.0, 0.0), axis=1, keepdims=True)
        used = (lane_slot == first) | (lane_slot == last)
        double = used & (first == last) & (count > 1.5)
        return jnp.where(used, jnp.where(double, BIAS, 0.0), UNUSED)

    bias = jnp.where(lane < slots, bias_of(me), bias_of(partner)).astype(bf16)

    pairs = steps * GROUPS // 2
    chunk = 512
    chunks = tokens // chunk
    queries, peaks, outs = {}, {}, {}
    for i in range(pairs + 2):
        if i < pairs:
            heads = [q_ref[:, (2 * i + j) * HD : (2 * i + j + 1) * HD] for j in range(2)]
            queries[i] = jnp.concatenate([jnp.concatenate([q, bias], axis=1) for q in heads], axis=0)
            peaks[i] = None
            if 2 * i % GROUPS == 0:
                loads[0, 2 * i // GROUPS].wait()
        if 0 <= i - 2 and 2 * (i - 2) % GROUPS == 0:
            loads[1, 2 * (i - 2) // GROUPS].wait()
        if 0 <= i - 1 < pairs:
            top = jnp.max(peaks[i - 1], axis=0, keepdims=True).astype(bf16)
            peaks[i - 1] = top.astype(f32)
            for h in range(2):
                g, head = divmod(2 * (i - 1) + h, GROUPS)
                for j in range(4):
                    out_ref[dest_of(g, head, j), 32:33, :] = top[:, h * rows : (h + 1) * rows]
        for k in range(chunks):
            at = slice(k * chunk, (k + 1) * chunk)
            if i < pairs:
                s = lax.dot_general(
                    kv_ref[2 * i // GROUPS, at, :], queries[i], (((1,), (1,)), ((), ())), preferred_element_type=f32
                )
                s_scr[i % 2, at, :] = s
                peak = jnp.max(s.reshape(chunk // 8, 8, 2 * rows), axis=0)
                peaks[i] = peak if peaks[i] is None else jnp.maximum(peaks[i], peak)
            if 0 <= i - 1 < pairs:
                n = i - 1
                p_scr[n % 2, at, :] = jnp.exp2((s_scr[n % 2, at, :] - peaks[n]) * RATE).astype(bf16)
            if 0 <= i - 2:
                n = i - 2
                tiles = [
                    kv_ref[2 * n // GROUPS, tokens + j * VROWS : tokens + (j + 1) * VROWS, :]
                    for j in range(k * chunk // TILE, (k + 1) * chunk // TILE)
                ]
                out = jnp.dot(jnp.concatenate(tiles, axis=1), p_scr[n % 2, at, :], preferred_element_type=f32)
                outs[n] = out if k == 0 else outs[n] + out
        if 0 <= i - 2:
            out = outs.pop(i - 2)
            for h in range(2):
                g, head = divmod(2 * (i - 2) + h, GROUPS)
                cols = slice(h * rows, (h + 1) * rows)
                total = out[HD : HD + 1, cols]
                high = total.astype(bf16)
                low = (total - high.astype(f32)).astype(bf16)
                for j in range(4):
                    dest = dest_of(g, head, j)
                    out_ref[dest, 0:32, :] = out[j * 32 : (j + 1) * 32, cols].astype(bf16)
                    out_ref[dest, 33:34, :] = high
                    out_ref[dest, 34:35, :] = low


def dest_of(g, h, j):
    return ((j % 2) * 4 + g * 2 + h // 4) * 8 + (h % 4) * 2 + j // 2


def merge_body(got_ref, out_ref):
    chips, _, rows = got_ref.shape
    peaks = [got_ref[i, 32:33, :].astype(f32) for i in range(chips)]
    top = functools.reduce(jnp.maximum, peaks)
    total = jnp.zeros((1, rows), f32)
    number = jnp.zeros((32, rows), f32)
    for i in range(chips):
        factor = jnp.exp2((peaks[i] - top) * RATE)
        total += factor * (got_ref[i, 33:34, :].astype(f32) + got_ref[i, 34:35, :].astype(f32))
        number += factor * got_ref[i, 0:32, :].astype(f32)
    attention = number / total
    high = attention.astype(bf16)
    out_ref[0:32, :] = high
    out_ref[32:64, :] = (attention - high.astype(f32)).astype(bf16)


def project_body(*refs):
    count = len(refs) // 2
    lefts, rights, out_ref = refs[:count], refs[count:-1], refs[-1]
    left = jnp.concatenate([r[...] for r in lefts], axis=0)
    step = 512
    for i in range(out_ref.shape[1] // step):
        cols = slice(i * step, (i + 1) * step)
        right = jnp.concatenate([r[:, cols] for r in rights for _ in range(2)], axis=0)
        part = lax.dot_general(left, right, (((0,), (0,)), ((), ())), preferred_element_type=f32)
        out_ref[:, cols] = part.astype(bf16)


def finish_body(got_ref, out_ref):
    devices, parts, part = got_ref.shape
    mates = out_ref.shape[1] // (parts * part)
    for m in range(mates):
        total = sum(got_ref[i].astype(f32) for i in range(m, devices, mates)).astype(bf16)
        for r in range(parts):
            at = (m * parts + r) * part
            out_ref[:, at : at + part] = total[r : r + 1]


def small_call(body, out, *args, scalars=(), scratch=(), mib=8, flops=0, large=0):
    smem = pl.BlockSpec(memory_space=pltpu.SMEM)
    vmem = pl.BlockSpec(memory_space=pltpu.VMEM)
    return pl.pallas_call(
        body,
        out_shape=out,
        in_specs=[smem] * len(scalars) + [vmem] * (len(args) - large) + [pl.BlockSpec(memory_space=pltpu.HBM)] * large,
        out_specs=jax.tree.map(lambda _: vmem, out),
        scratch_shapes=list(scratch),
        cost_estimate=pl.CostEstimate(flops=flops, transcendentals=0, bytes_accessed=0) if flops else None,
        compiler_params=pltpu.CompilerParams(vmem_limit_bytes=mib << 20),
        interpret=INTERPRET,
    )(*scalars, *args)


def swapped(v):
    return lax.ppermute(v, "c", [(0, 1), (1, 0)])


def to_mate(v, k):
    nx, nc = lax.axis_size("x"), lax.axis_size("c")
    perm = [(x * nc + c, (x ^ (k // nc)) * nc + (c ^ (k % nc))) for x in range(nx) for c in range(nc)]
    return lax.ppermute(v, ("x", "c"), perm)


def to_owner(v, k):
    ny, nx, nc = (lax.axis_size(a) for a in POOL)
    pairs = []
    for half in range(nc):
        for y in range(ny // nc):
            for x in range(nx):
                for c in range(nc):
                    source = ((half * (ny // nc) + y) * nx + x) * nc + c
                    target = ((c * (ny // nc) + y) * nx + (x ^ (k // nc))) * nc + (half ^ (k % nc))
                    pairs.append((source, target))
    return lax.ppermute(v, POOL, pairs)


def per_device(query, kv_pool, holder_table, slot_table, lengths, out_weight):
    ny, nx, nc = (lax.axis_size(a) for a in POOL)
    y, x, c = (lax.axis_index(a) for a in POOL)
    chips = ny * nx
    pos = jnp.stack([(y * nx + x) * nc + c, c]).astype(jnp.int32)

    devices = chips * nc
    width = HALF + 2 * holder_table.shape[1]
    row_shape = jax.ShapeDtypeStruct((devices, 2, width // 2), bf16)
    scratch = [pltpu.VMEM(v.shape, v.dtype) for v in (query, holder_table, slot_table)]
    rows = small_call(
        row_body,
        row_shape,
        query,
        holder_table,
        slot_table,
        scalars=(lengths,),
        scratch=[*scratch, pltpu.SemaphoreType.DMA((3,))],
        large=3,
        mib=62,
    )
    q = lax.all_to_all(rows, POOL, split_axis=0, concat_axis=0, tiled=True)

    kv_other = swapped(kv_pool)
    tokens = nc * kv_pool.shape[0] * kv_pool.shape[2]
    steps = KVH // nc
    kv_shape = (steps, tokens + tokens // TILE * VROWS, TILE)
    blocks = small_call(
        blocks_body, jax.ShapeDtypeStruct(kv_shape, bf16), kv_pool, kv_other, scalars=(pos,), flops=1 << 32
    )

    mates = 2 * nc
    mate = (x % 2) * nc + c
    d_part = out_weight.shape[1] // mates
    weights = []
    for k in range(mates):
        part = lax.dynamic_slice_in_dim(out_weight, (mate ^ k) * d_part, d_part, axis=1)
        weights.append(to_mate(part, k) if k else part)

    q = q.reshape(devices, width)
    parts = small_call(
        attention_body,
        jax.ShapeDtypeStruct((chips, 40, devices), bf16),
        q,
        blocks,
        scalars=(pos,),
        scratch=[
            pltpu.VMEM(kv_shape, bf16),
            pltpu.VMEM((2, tokens, 2 * devices), f32),
            pltpu.VMEM((2, tokens, 2 * devices), bf16),
            pltpu.SemaphoreType.DMA((2, steps)),
        ],
        mib=52,
        large=1,
        flops=1 << 34,
    )
    parts = lax.all_to_all(parts, CHIPS, split_axis=0, concat_axis=0, tiled=True)
    mine = small_call(merge_body, jax.ShapeDtypeStruct((64, devices), bf16), parts)
    lefts = [to_owner(mine, k) for k in range(mates)]
    partial = small_call(project_body, jax.ShapeDtypeStruct((devices, d_part), bf16), *lefts, *weights)
    columns = lax.all_to_all(
        partial.reshape(devices, 2, d_part // 2), POOL, split_axis=0, concat_axis=0, tiled=True
    )
    return small_call(finish_body, jax.ShapeDtypeStruct((1, mates * d_part), bf16), columns)


def solution(mesh):
    torus = Mesh(mesh.devices.reshape(mesh.shape["grp"], 8, 8, 2), GRP_POOL)
    return jax.shard_map(
        per_device,
        mesh=torus,
        in_specs=(
            P(GRP_POOL, None),
            P(GRP_POOL, None, None, None),
            P(GRP_POOL, None),
            P(GRP_POOL, None),
            P(GRP_POOL),
            P(POOL, None),
        ),
        out_specs=P(GRP_POOL, None),
        check_vma=False,
    )
```

```python
import functools
import math

import jax
import jax.numpy as jnp
from jax import lax
from jax.experimental import pallas as pl
from jax.experimental.pallas import tpu as pltpu
from jax.sharding import Mesh
from jax.sharding import PartitionSpec as P


H = 32
KVH = 4
HD = 128
GROUPS = H // KVH
CORES = 2
POOL = ("y", "x", "c")
CHIPS = ("y", "x")
GRP_POOL = ("grp", "y", "x", "c")
RATE = math.log2(math.e) / math.sqrt(HD)
TWICE = math.log(2.0) * math.sqrt(HD)
UNUSED = -32768.0
HALF = H * HD // CORES
TILE = 2 * HD
VROWS = HD + 16
INTERPRET = False

f32 = jnp.float32
bf16 = jnp.bfloat16


def as_product(value):
    pairs = []
    for i in range(128):
        mark = 1.0 + i / 128.0
        unit = 2.0 ** (math.floor(math.log2(value / mark)) - 7)
        bias = round(value / mark / unit) * unit
        pairs.append((abs(mark * bias - value), mark, bias))
    return min(pairs)[1:]


MARK, BIAS = as_product(TWICE)


def row_body(length_ref, q_hbm, holder_hbm, slot_hbm, out_ref, q_ref, holder_ref, slot_ref, sems):
    pairs = ((q_hbm, q_ref), (holder_hbm, holder_ref), (slot_hbm, slot_ref))
    loads = [pltpu.make_async_copy(source, target, sems.at[n]) for n, (source, target) in enumerate(pairs)]
    for load in loads:
        load.start()
    for load in loads:
        load.wait()
    devices, _, part = out_ref.shape
    lane = lax.broadcasted_iota(jnp.int32, holder_ref.shape, 1)
    holder = jnp.where(lane < length_ref[0], holder_ref[...], -1).astype(f32)
    table = [holder, slot_ref[...].astype(f32)]
    for core in range(CORES):
        row = jnp.concatenate([q_ref[:, core * HALF : (core + 1) * HALF].astype(f32)] + table, axis=1)
        row = jnp.concatenate([row[:, :part], row[:, part:]], axis=0).astype(bf16)

        def put(i, carry, row=row, core=core):
            out_ref[i * CORES + core] = row
            return carry

        lax.fori_loop(0, devices // CORES, put, 0)


def blocks_body(pos_ref, own_ref, other_ref, out_ref):
    slots, _, blk, _ = own_ref.shape
    tokens = slots * blk
    token_slot = lax.broadcasted_iota(jnp.int32, (2 * tokens, HD), 0) // blk
    slot_lane = lax.broadcasted_iota(jnp.int32, (2 * tokens, HD), 1)
    mark = jnp.where(slot_lane == token_slot, MARK, 0.0).astype(bf16)
    for g in range(KVH // CORES):
        out_ref[g, : 2 * tokens, HD:] = mark
        at = pl.ds(pl.multiple_of((pos_ref[1] * (KVH // CORES) + g) * HD, HD), HD)
        for i, ref in enumerate((own_ref, other_ref)):
            out_ref[g, i * tokens : (i + 1) * tokens, :HD] = ref[:, 0, :, at].reshape(tokens, HD)
            turned = ref[:, 1, :, at].reshape(tokens, HD).T
            for j in range(tokens // TILE):
                row = 2 * tokens + (i * (tokens // TILE) + j) * VROWS
                out_ref[g, row : row + HD, :] = turned[:, j * TILE : (j + 1) * TILE]
                out_ref[g, row + HD : row + VROWS, :] = jnp.ones((VROWS - HD, TILE), bf16)


def attention_body(pos_ref, q_ref, kv_hbm, out_ref, kv_ref, s_scr, p_scr, sems):
    rows = q_ref.shape[0]
    steps = kv_ref.shape[0]
    tokens = s_scr.shape[1]
    loads = {}
    for g in range(steps):
        for n, at in enumerate((slice(0, tokens), slice(tokens, kv_ref.shape[1]))):
            loads[n, g] = pltpu.make_async_copy(kv_hbm.at[g, at], kv_ref.at[g, at], sems.at[n, g])
            loads[n, g].start()
    slots = HD // 2
    me, core = pos_ref[0], pos_ref[1]
    partner = me + 1 - 2 * core
    holder = q_ref[:, HALF : HALF + HD].astype(f32)
    slot = q_ref[:, HALF + HD : HALF + 2 * HD].astype(f32)
    lane = lax.broadcasted_iota(jnp.int32, (rows, HD), 1)
    lane_slot = jnp.where(lane < slots, lane, lane - slots).astype(f32)

    def bias_of(device):
        hit = holder == device.astype(f32)
        first = jnp.min(jnp.where(hit, slot, 999.0), axis=1, keepdims=True)
        last = jnp.max(jnp.where(hit, slot, -1.0), axis=1, keepdims=True)
        count = jnp.sum(jnp.where(hit, 1.0, 0.0), axis=1, keepdims=True)
        used = (lane_slot == first) | (lane_slot == last)
        double = used & (first == last) & (count > 1.5)
        return jnp.where(used, jnp.where(double, BIAS, 0.0), UNUSED)

    bias = jnp.where(lane < slots, bias_of(me), bias_of(partner)).astype(bf16)

    pairs = steps * GROUPS // 2
    chunk = 512
    chunks = tokens // chunk
    queries, peaks, outs = {}, {}, {}
    for i in range(pairs + 2):
        if i < pairs:
            heads = [q_ref[:, (2 * i + j) * HD : (2 * i + j + 1) * HD] for j in range(2)]
            queries[i] = jnp.concatenate([jnp.concatenate([q, bias], axis=1) for q in heads], axis=0)
            peaks[i] = None
            if 2 * i % GROUPS == 0:
                loads[0, 2 * i // GROUPS].wait()
        if 0 <= i - 2 and 2 * (i - 2) % GROUPS == 0:
            loads[1, 2 * (i - 2) // GROUPS].wait()
        if 0 <= i - 1 < pairs:
            top = jnp.max(peaks[i - 1], axis=0, keepdims=True).astype(bf16)
            peaks[i - 1] = top.astype(f32)
            for h in range(2):
                g, head = divmod(2 * (i - 1) + h, GROUPS)
                for j in range(4):
                    out_ref[dest_of(g, head, j), 32:33, :] = top[:, h * rows : (h + 1) * rows]
        for k in range(chunks):
            at = slice(k * chunk, (k + 1) * chunk)
            if i < pairs:
                s = lax.dot_general(
                    kv_ref[2 * i // GROUPS, at, :], queries[i], (((1,), (1,)), ((), ())), preferred_element_type=f32
                )
                s_scr[i % 2, at, :] = s
                peak = jnp.max(s.reshape(chunk // 8, 8, 2 * rows), axis=0)
                peaks[i] = peak if peaks[i] is None else jnp.maximum(peaks[i], peak)
            if 0 <= i - 1 < pairs:
                n = i - 1
                p_scr[n % 2, at, :] = jnp.exp2((s_scr[n % 2, at, :] - peaks[n]) * RATE).astype(bf16)
            if 0 <= i - 2:
                n = i - 2
                tiles = [
                    kv_ref[2 * n // GROUPS, tokens + j * VROWS : tokens + (j + 1) * VROWS, :]
                    for j in range(k * chunk // TILE, (k + 1) * chunk // TILE)
                ]
                out = jnp.dot(jnp.concatenate(tiles, axis=1), p_scr[n % 2, at, :], preferred_element_type=f32)
                outs[n] = out if k == 0 else outs[n] + out
        if 0 <= i - 2:
            out = outs.pop(i - 2)
            for h in range(2):
                g, head = divmod(2 * (i - 2) + h, GROUPS)
                cols = slice(h * rows, (h + 1) * rows)
                total = out[HD : HD + 1, cols]
                high = total.astype(bf16)
                low = (total - high.astype(f32)).astype(bf16)
                for j in range(4):
                    dest = dest_of(g, head, j)
                    out_ref[dest, 0:32, :] = out[j * 32 : (j + 1) * 32, cols].astype(bf16)
                    out_ref[dest, 33:34, :] = high
                    out_ref[dest, 34:35, :] = low


def dest_of(g, h, j):
    return ((j % 2) * 4 + g * 2 + h // 4) * 8 + (h % 4) * 2 + j // 2


def merge_body(got_ref, out_ref):
    chips, _, rows = got_ref.shape
    peaks = [got_ref[i, 32:33, :].astype(f32) for i in range(chips)]
    top = functools.reduce(jnp.maximum, peaks)
    total = jnp.zeros((1, rows), f32)
    number = jnp.zeros((32, rows), f32)
    for i in range(chips):
        factor = jnp.exp2((peaks[i] - top) * RATE)
        total += factor * (got_ref[i, 33:34, :].astype(f32) + got_ref[i, 34:35, :].astype(f32))
        number += factor * got_ref[i, 0:32, :].astype(f32)
    attention = number / total
    high = attention.astype(bf16)
    out_ref[0:32, :] = high
    out_ref[32:64, :] = (attention - high.astype(f32)).astype(bf16)


def project_body(*refs):
    count = len(refs) // 2
    lefts, rights, out_ref = refs[:count], refs[count:-1], refs[-1]
    left = jnp.concatenate([r[...] for r in lefts], axis=0)
    step = 512
    for i in range(out_ref.shape[1] // step):
        cols = slice(i * step, (i + 1) * step)
        right = jnp.concatenate([r[:, cols] for r in rights for _ in range(2)], axis=0)
        part = lax.dot_general(left, right, (((0,), (0,)), ((), ())), preferred_element_type=f32)
        out_ref[:, cols] = part.astype(bf16)


def finish_body(got_ref, out_ref):
    devices, parts, part = got_ref.shape
    mates = out_ref.shape[1] // (parts * part)
    for m in range(mates):
        total = sum(got_ref[i].astype(f32) for i in range(m, devices, mates)).astype(bf16)
        for r in range(parts):
            at = (m * parts + r) * part
            out_ref[:, at : at + part] = total[r : r + 1]


def small_call(body, out, *args, scalars=(), scratch=(), mib=8, flops=0, large=0):
    smem = pl.BlockSpec(memory_space=pltpu.SMEM)
    vmem = pl.BlockSpec(memory_space=pltpu.VMEM)
    return pl.pallas_call(
        body,
        out_shape=out,
        in_specs=[smem] * len(scalars) + [vmem] * (len(args) - large) + [pl.BlockSpec(memory_space=pltpu.HBM)] * large,
        out_specs=jax.tree.map(lambda _: vmem, out),
        scratch_shapes=list(scratch),
        cost_estimate=pl.CostEstimate(flops=flops, transcendentals=0, bytes_accessed=0) if flops else None,
        compiler_params=pltpu.CompilerParams(vmem_limit_bytes=mib << 20),
        interpret=INTERPRET,
    )(*scalars, *args)


def swapped(v):
    return lax.ppermute(v, "c", [(0, 1), (1, 0)])


def to_mate(v, k):
    nx, nc = lax.axis_size("x"), lax.axis_size("c")
    perm = [(x * nc + c, (x ^ (k // nc)) * nc + (c ^ (k % nc))) for x in range(nx) for c in range(nc)]
    return lax.ppermute(v, ("x", "c"), perm)


def to_owner(v, k):
    ny, nx, nc = (lax.axis_size(a) for a in POOL)
    pairs = []
    for half in range(nc):
        for y in range(ny // nc):
            for x in range(nx):
                for c in range(nc):
                    source = ((half * (ny // nc) + y) * nx + x) * nc + c
                    target = ((c * (ny // nc) + y) * nx + (x ^ (k // nc))) * nc + (half ^ (k % nc))
                    pairs.append((source, target))
    return lax.ppermute(v, POOL, pairs)


def per_device(query, kv_pool, holder_table, slot_table, lengths, out_weight):
    ny, nx, nc = (lax.axis_size(a) for a in POOL)
    y, x, c = (lax.axis_index(a) for a in POOL)
    chips = ny * nx
    pos = jnp.stack([(y * nx + x) * nc + c, c]).astype(jnp.int32)

    devices = chips * nc
    width = HALF + 2 * holder_table.shape[1]
    row_shape = jax.ShapeDtypeStruct((devices, 2, width // 2), bf16)
    scratch = [pltpu.VMEM(v.shape, v.dtype) for v in (query, holder_table, slot_table)]
    rows = small_call(
        row_body,
        row_shape,
        query,
        holder_table,
        slot_table,
        scalars=(lengths,),
        scratch=[*scratch, pltpu.SemaphoreType.DMA((3,))],
        large=3,
        mib=62,
    )
    q = lax.all_to_all(rows, POOL, split_axis=0, concat_axis=0, tiled=True)

    kv_other = swapped(kv_pool)
    tokens = nc * kv_pool.shape[0] * kv_pool.shape[2]
    steps = KVH // nc
    kv_shape = (steps, tokens + tokens // TILE * VROWS, TILE)
    blocks = small_call(
        blocks_body, jax.ShapeDtypeStruct(kv_shape, bf16), kv_pool, kv_other, scalars=(pos,), flops=1 << 32
    )

    mates = 2 * nc
    first = (x % 2) * nc + y // (ny // nc)
    d_part = out_weight.shape[1] // mates
    weights = []
    for k in range(mates):
        part = lax.dynamic_slice_in_dim(out_weight, (first ^ k) * d_part, d_part, axis=1)
        weights.append(to_owner(part, k))

    q = q.reshape(devices, width)
    parts = small_call(
        attention_body,
        jax.ShapeDtypeStruct((chips, 40, devices), bf16),
        q,
        blocks,
        scalars=(pos,),
        scratch=[
            pltpu.VMEM(kv_shape, bf16),
            pltpu.VMEM((2, tokens, 2 * devices), f32),
            pltpu.VMEM((2, tokens, 2 * devices), bf16),
            pltpu.SemaphoreType.DMA((2, steps)),
        ],
        mib=52,
        large=1,
        flops=1 << 34,
    )
    parts = lax.all_to_all(parts, CHIPS, split_axis=0, concat_axis=0, tiled=True)
    mine = small_call(merge_body, jax.ShapeDtypeStruct((64, devices), bf16), parts)
    lefts = [to_mate(mine, k) if k else mine for k in range(mates)]
    partial = small_call(project_body, jax.ShapeDtypeStruct((devices, d_part), bf16), *lefts, *weights)
    columns = lax.all_to_all(
        partial.reshape(devices, 2, d_part // 2), POOL, split_axis=0, concat_axis=0, tiled=True
    )
    return small_call(finish_body, jax.ShapeDtypeStruct((1, mates * d_part), bf16), columns)


def solution(mesh):
    torus = Mesh(mesh.devices.reshape(mesh.shape["grp"], 8, 8, 2), GRP_POOL)
    return jax.shard_map(
        per_device,
        mesh=torus,
        in_specs=(
            P(GRP_POOL, None),
            P(GRP_POOL, None, None, None),
            P(GRP_POOL, None),
            P(GRP_POOL, None),
            P(GRP_POOL),
            P(POOL, None),
        ),
        out_specs=P(GRP_POOL, None),
        check_vma=False,
    )
```

```python
import functools
import math

import jax
import jax.numpy as jnp
from jax import lax
from jax.experimental import pallas as pl
from jax.experimental.pallas import tpu as pltpu
from jax.sharding import Mesh
from jax.sharding import PartitionSpec as P


H = 32
KVH = 4
HD = 128
GROUPS = H // KVH
CORES = 2
POOL = ("y", "x", "c")
CHIPS = ("y", "x")
GRP_POOL = ("grp", "y", "x", "c")
RATE = math.log2(math.e) / math.sqrt(HD)
TWICE = math.log(2.0) * math.sqrt(HD)
UNUSED = -32768.0
HALF = H * HD // CORES
TILE = 2 * HD
VROWS = HD + 16
SLICE = 32
INTERPRET = False

f32 = jnp.float32
bf16 = jnp.bfloat16


def as_product(value):
    pairs = []
    for i in range(128):
        mark = 1.0 + i / 128.0
        unit = 2.0 ** (math.floor(math.log2(value / mark)) - 7)
        bias = round(value / mark / unit) * unit
        pairs.append((abs(mark * bias - value), mark, bias))
    return min(pairs)[1:]


MARK, BIAS = as_product(TWICE)


def row_body(length_ref, q_hbm, holder_hbm, slot_hbm, out_ref, q_ref, holder_ref, slot_ref, sems):
    pairs = ((q_hbm, q_ref), (holder_hbm, holder_ref), (slot_hbm, slot_ref))
    loads = [pltpu.make_async_copy(source, target, sems.at[n]) for n, (source, target) in enumerate(pairs)]
    for load in loads:
        load.start()
    for load in loads:
        load.wait()
    devices, _, part = out_ref.shape
    lane = lax.broadcasted_iota(jnp.int32, holder_ref.shape, 1)
    holder = jnp.where(lane < length_ref[0], holder_ref[...], -1).astype(f32)
    table = [holder, slot_ref[...].astype(f32)]
    for core in range(CORES):
        row = jnp.concatenate([q_ref[:, core * HALF : (core + 1) * HALF].astype(f32)] + table, axis=1)
        row = jnp.concatenate([row[:, :part], row[:, part:]], axis=0).astype(bf16)

        def put(i, carry, row=row, core=core):
            out_ref[i * CORES + core] = row
            return carry

        lax.fori_loop(0, devices // CORES, put, 0)


def blocks_body(pos_ref, own_ref, other_ref, out_ref):
    slots, _, blk, _ = own_ref.shape
    tokens = slots * blk
    token_slot = lax.broadcasted_iota(jnp.int32, (2 * tokens, HD), 0) // blk
    slot_lane = lax.broadcasted_iota(jnp.int32, (2 * tokens, HD), 1)
    mark = jnp.where(slot_lane == token_slot, MARK, 0.0).astype(bf16)
    for g in range(KVH // CORES):
        out_ref[g, : 2 * tokens, HD:] = mark
        at = pl.ds(pl.multiple_of((pos_ref[1] * (KVH // CORES) + g) * HD, HD), HD)
        for i, ref in enumerate((own_ref, other_ref)):
            out_ref[g, i * tokens : (i + 1) * tokens, :HD] = ref[:, 0, :, at].reshape(tokens, HD)
            turned = ref[:, 1, :, at].reshape(tokens, HD).T
            for j in range(tokens // TILE):
                row = 2 * tokens + (i * (tokens // TILE) + j) * VROWS
                out_ref[g, row : row + HD, :] = turned[:, j * TILE : (j + 1) * TILE]
                out_ref[g, row + HD : row + VROWS, :] = jnp.ones((VROWS - HD, TILE), bf16)


def attention_body(pos_ref, q_ref, kv_hbm, out_ref, kv_ref, s_scr, p_scr, sems):
    rows = q_ref.shape[0]
    steps = kv_ref.shape[0]
    tokens = s_scr.shape[1]
    loads = {}
    for g in range(steps):
        for n, at in enumerate((slice(0, tokens), slice(tokens, kv_ref.shape[1]))):
            loads[n, g] = pltpu.make_async_copy(kv_hbm.at[g, at], kv_ref.at[g, at], sems.at[n, g])
            loads[n, g].start()
    slots = HD // 2
    me, core = pos_ref[0], pos_ref[1]
    partner = me + 1 - 2 * core
    holder = q_ref[:, HALF : HALF + HD].astype(f32)
    slot = q_ref[:, HALF + HD : HALF + 2 * HD].astype(f32)
    lane = lax.broadcasted_iota(jnp.int32, (rows, HD), 1)
    lane_slot = jnp.where(lane < slots, lane, lane - slots).astype(f32)

    def bias_of(device):
        hit = holder == device.astype(f32)
        first = jnp.min(jnp.where(hit, slot, 999.0), axis=1, keepdims=True)
        last = jnp.max(jnp.where(hit, slot, -1.0), axis=1, keepdims=True)
        count = jnp.sum(jnp.where(hit, 1.0, 0.0), axis=1, keepdims=True)
        used = (lane_slot == first) | (lane_slot == last)
        double = used & (first == last) & (count > 1.5)
        return jnp.where(used, jnp.where(double, BIAS, 0.0), UNUSED)

    bias = jnp.where(lane < slots, bias_of(me), bias_of(partner)).astype(bf16)

    pairs = steps * GROUPS // 2
    chunk = 512
    chunks = tokens // chunk
    queries, peaks, outs = {}, {}, {}
    for i in range(pairs + 2):
        if i < pairs:
            heads = [q_ref[:, (2 * i + j) * HD : (2 * i + j + 1) * HD] for j in range(2)]
            queries[i] = jnp.concatenate([jnp.concatenate([q, bias], axis=1) for q in heads], axis=0)
            peaks[i] = None
            if 2 * i % GROUPS == 0:
                loads[0, 2 * i // GROUPS].wait()
        if 0 <= i - 2 and 2 * (i - 2) % GROUPS == 0:
            loads[1, 2 * (i - 2) // GROUPS].wait()
        if 0 <= i - 1 < pairs:
            top = jnp.max(peaks[i - 1], axis=0, keepdims=True).astype(bf16)
            peaks[i - 1] = top.astype(f32)
        for k in range(chunks):
            at = slice(k * chunk, (k + 1) * chunk)
            if i < pairs:
                s = lax.dot_general(
                    kv_ref[2 * i // GROUPS, at, :], queries[i], (((1,), (1,)), ((), ())), preferred_element_type=f32
                )
                s_scr[i % 2, at, :] = s
                peak = jnp.max(s.reshape(chunk // 8, 8, 2 * rows), axis=0)
                peaks[i] = peak if peaks[i] is None else jnp.maximum(peaks[i], peak)
            if 0 <= i - 1 < pairs:
                n = i - 1
                p_scr[n % 2, at, :] = jnp.exp2((s_scr[n % 2, at, :] - peaks[n]) * RATE).astype(bf16)
            if 0 <= i - 2:
                n = i - 2
                tiles = [
                    kv_ref[2 * n // GROUPS, tokens + j * VROWS : tokens + (j + 1) * VROWS, :]
                    for j in range(k * chunk // TILE, (k + 1) * chunk // TILE)
                ]
                out = jnp.dot(jnp.concatenate(tiles, axis=1), p_scr[n % 2, at, :], preferred_element_type=f32)
                outs[n] = out if k == 0 else outs[n] + out
        if 0 <= i - 2:
            out = outs.pop(i - 2)
            for h in range(2):
                g, head = divmod(2 * (i - 2) + h, GROUPS)
                cols = slice(h * rows, (h + 1) * rows)
                stat = jnp.concatenate([peaks[i - 2][:, cols], out[HD : HD + 1, cols]], axis=0).astype(bf16)
                for j in range(4):
                    dest = dest_of(g, head, j)
                    for t in range(SLICE // 2):
                        pair = out[j * SLICE + 2 * t : j * SLICE + 2 * t + 2, cols]
                        out_ref[dest, :, t * rows : (t + 1) * rows] = pair.astype(bf16)
                    out_ref[dest, :, SLICE // 2 * rows :] = stat


def dest_of(g, h, j):
    return ((j % 2) * 4 + g * 2 + h // 4) * 8 + (h % 4) * 2 + j // 2


def merge_body(got_ref, out_ref):
    chips, _, _ = got_ref.shape
    rows = out_ref.shape[1]
    pairs = SLICE // 2
    stats = [got_ref[i, :, pairs * rows :].astype(f32) for i in range(chips)]
    top = functools.reduce(jnp.maximum, [s[:1] for s in stats])
    total = jnp.zeros((1, rows), f32)
    number = jnp.zeros((2, pairs * rows), f32)
    for i in range(chips):
        factor = jnp.exp2((stats[i][:1] - top) * RATE)
        total += factor * stats[i][1:]
        number += jnp.concatenate([factor] * pairs, axis=1) * got_ref[i, :, : pairs * rows].astype(f32)
    attention = number / jnp.concatenate([total] * pairs, axis=1)
    attention = jnp.concatenate([attention[:, t * rows : (t + 1) * rows] for t in range(pairs)], axis=0)
    high = attention.astype(bf16)
    out_ref[:SLICE, :] = high
    out_ref[SLICE:, :] = (attention - high.astype(f32)).astype(bf16)


def project_body(*refs):
    count = len(refs) // 2
    lefts, rights, out_ref = refs[:count], refs[count:-1], refs[-1]
    left = jnp.concatenate([r[...] for r in lefts], axis=0)
    step = 512
    for i in range(out_ref.shape[1] // step):
        cols = slice(i * step, (i + 1) * step)
        right = jnp.concatenate([r[:, cols] for r in rights for _ in range(2)], axis=0)
        part = lax.dot_general(left, right, (((0,), (0,)), ((), ())), preferred_element_type=f32)
        out_ref[:, cols] = part.astype(bf16)


def finish_body(got_ref, out_ref):
    devices, parts, part = got_ref.shape
    mates = out_ref.shape[1] // (parts * part)
    for m in range(mates):
        total = sum(got_ref[i].astype(f32) for i in range(m, devices, mates)).astype(bf16)
        for r in range(parts):
            at = (m * parts + r) * part
            out_ref[:, at : at + part] = total[r : r + 1]


def small_call(body, out, *args, scalars=(), scratch=(), mib=8, flops=0, large=0):
    smem = pl.BlockSpec(memory_space=pltpu.SMEM)
    vmem = pl.BlockSpec(memory_space=pltpu.VMEM)
    return pl.pallas_call(
        body,
        out_shape=out,
        in_specs=[smem] * len(scalars) + [vmem] * (len(args) - large) + [pl.BlockSpec(memory_space=pltpu.HBM)] * large,
        out_specs=jax.tree.map(lambda _: vmem, out),
        scratch_shapes=list(scratch),
        cost_estimate=pl.CostEstimate(flops=flops, transcendentals=0, bytes_accessed=0) if flops else None,
        compiler_params=pltpu.CompilerParams(vmem_limit_bytes=mib << 20),
        interpret=INTERPRET,
    )(*scalars, *args)


def swapped(v):
    return lax.ppermute(v, "c", [(0, 1), (1, 0)])


def to_mate(v, k):
    nx, nc = lax.axis_size("x"), lax.axis_size("c")
    perm = [(x * nc + c, (x ^ (k // nc)) * nc + (c ^ (k % nc))) for x in range(nx) for c in range(nc)]
    return lax.ppermute(v, ("x", "c"), perm)


def to_owner(v, k):
    ny, nx, nc = (lax.axis_size(a) for a in POOL)
    pairs = []
    for half in range(nc):
        for y in range(ny // nc):
            for x in range(nx):
                for c in range(nc):
                    source = ((half * (ny // nc) + y) * nx + x) * nc + c
                    target = ((c * (ny // nc) + y) * nx + (x ^ (k // nc))) * nc + (half ^ (k % nc))
                    pairs.append((source, target))
    return lax.ppermute(v, POOL, pairs)


def per_device(query, kv_pool, holder_table, slot_table, lengths, out_weight):
    ny, nx, nc = (lax.axis_size(a) for a in POOL)
    y, x, c = (lax.axis_index(a) for a in POOL)
    chips = ny * nx
    pos = jnp.stack([(y * nx + x) * nc + c, c]).astype(jnp.int32)

    devices = chips * nc
    width = HALF + 2 * holder_table.shape[1]
    row_shape = jax.ShapeDtypeStruct((devices, 2, width // 2), bf16)
    scratch = [pltpu.VMEM(v.shape, v.dtype) for v in (query, holder_table, slot_table)]
    rows = small_call(
        row_body,
        row_shape,
        query,
        holder_table,
        slot_table,
        scalars=(lengths,),
        scratch=[*scratch, pltpu.SemaphoreType.DMA((3,))],
        large=3,
        mib=62,
    )
    q = lax.all_to_all(rows, POOL, split_axis=0, concat_axis=0, tiled=True)

    kv_other = swapped(kv_pool)
    tokens = nc * kv_pool.shape[0] * kv_pool.shape[2]
    steps = KVH // nc
    kv_shape = (steps, tokens + tokens // TILE * VROWS, TILE)
    blocks = small_call(
        blocks_body, jax.ShapeDtypeStruct(kv_shape, bf16), kv_pool, kv_other, scalars=(pos,), flops=1 << 32
    )

    mates = 2 * nc
    first = (x % 2) * nc + y // (ny // nc)
    d_part = out_weight.shape[1] // mates
    weights = []
    for k in range(mates):
        part = lax.dynamic_slice_in_dim(out_weight, (first ^ k) * d_part, d_part, axis=1)
        weights.append(to_owner(part, k))

    q = q.reshape(devices, width)
    parts = small_call(
        attention_body,
        jax.ShapeDtypeStruct((chips, 2, (SLICE // 2 + 1) * devices), bf16),
        q,
        blocks,
        scalars=(pos,),
        scratch=[
            pltpu.VMEM(kv_shape, bf16),
            pltpu.VMEM((2, tokens, 2 * devices), f32),
            pltpu.VMEM((2, tokens, 2 * devices), bf16),
            pltpu.SemaphoreType.DMA((2, steps)),
        ],
        mib=52,
        large=1,
        flops=1 << 34,
    )
    parts = lax.all_to_all(parts, CHIPS, split_axis=0, concat_axis=0, tiled=True)
    mine = small_call(merge_body, jax.ShapeDtypeStruct((2 * SLICE, devices), bf16), parts)
    lefts = [to_mate(mine, k) if k else mine for k in range(mates)]
    partial = small_call(project_body, jax.ShapeDtypeStruct((devices, d_part), bf16), *lefts, *weights)
    columns = lax.all_to_all(
        partial.reshape(devices, 2, d_part // 2), POOL, split_axis=0, concat_axis=0, tiled=True
    )
    return small_call(finish_body, jax.ShapeDtypeStruct((1, mates * d_part), bf16), columns)


def solution(mesh):
    torus = Mesh(mesh.devices.reshape(mesh.shape["grp"], 8, 8, 2), GRP_POOL)
    return jax.shard_map(
        per_device,
        mesh=torus,
        in_specs=(
            P(GRP_POOL, None),
            P(GRP_POOL, None, None, None),
            P(GRP_POOL, None),
            P(GRP_POOL, None),
            P(GRP_POOL),
            P(POOL, None),
        ),
        out_specs=P(GRP_POOL, None),
        check_vma=False,
    )
```

```python
import functools
import math

import jax
import jax.numpy as jnp
from jax import lax
from jax.experimental import pallas as pl
from jax.experimental.pallas import tpu as pltpu
from jax.sharding import Mesh
from jax.sharding import PartitionSpec as P


H = 32
KVH = 4
HD = 128
GROUPS = H // KVH
CORES = 2
POOL = ("y", "x", "c")
CHIPS = ("y", "x")
GRP_POOL = ("grp", "y", "x", "c")
RATE = math.log2(math.e) / math.sqrt(HD)
TWICE = math.log(2.0) * math.sqrt(HD)
UNUSED = -32768.0
HALF = H * HD // CORES
TILE = 2 * HD
VROWS = HD + 16
SLICE = 32
CHUNK = 512
INTERPRET = False

f32 = jnp.float32
bf16 = jnp.bfloat16


def as_product(value):
    pairs = []
    for i in range(128):
        mark = 1.0 + i / 128.0
        unit = 2.0 ** (math.floor(math.log2(value / mark)) - 7)
        bias = round(value / mark / unit) * unit
        pairs.append((abs(mark * bias - value), mark, bias))
    return min(pairs)[1:]


MARK, BIAS = as_product(TWICE)


def row_body(length_ref, q_hbm, holder_hbm, slot_hbm, out_ref, q_ref, holder_ref, slot_ref, sems):
    pairs = ((q_hbm, q_ref), (holder_hbm, holder_ref), (slot_hbm, slot_ref))
    loads = [pltpu.make_async_copy(source, target, sems.at[n]) for n, (source, target) in enumerate(pairs)]
    for load in loads:
        load.start()
    for load in loads:
        load.wait()
    devices, _, part = out_ref.shape
    lane = lax.broadcasted_iota(jnp.int32, holder_ref.shape, 1)
    holder = jnp.where(lane < length_ref[0], holder_ref[...], -1).astype(f32)
    table = [holder, slot_ref[...].astype(f32)]
    for core in range(CORES):
        row = jnp.concatenate([q_ref[:, core * HALF : (core + 1) * HALF].astype(f32)] + table, axis=1)
        row = jnp.concatenate([row[:, :part], row[:, part:]], axis=0).astype(bf16)

        def put(i, carry, row=row, core=core):
            out_ref[i * CORES + core] = row
            return carry

        lax.fori_loop(0, devices // CORES, put, 0)


def blocks_body(pos_ref, own_ref, other_ref, out_ref):
    slots, _, blk, _ = own_ref.shape
    tokens = slots * blk
    token_slot = lax.broadcasted_iota(jnp.int32, (2 * tokens, HD), 0) // blk
    slot_lane = lax.broadcasted_iota(jnp.int32, (2 * tokens, HD), 1)
    mark = jnp.where(slot_lane == token_slot, MARK, 0.0).astype(bf16)
    for g in range(KVH // CORES):
        out_ref[g, : 2 * tokens, HD:] = mark
        at = pl.ds(pl.multiple_of((pos_ref[1] * (KVH // CORES) + g) * HD, HD), HD)
        for i, ref in enumerate((own_ref, other_ref)):
            out_ref[g, i * tokens : (i + 1) * tokens, :HD] = ref[:, 0, :, at].reshape(tokens, HD)
            turned = ref[:, 1, :, at].reshape(tokens, HD).T
            for j in range(tokens // TILE):
                row = 2 * tokens + (i * (tokens // TILE) + j) * VROWS
                out_ref[g, row : row + HD, :] = turned[:, j * TILE : (j + 1) * TILE]
                out_ref[g, row + HD : row + VROWS, :] = jnp.ones((VROWS - HD, TILE), bf16)


def attention_body(pos_ref, q_ref, kv_hbm, out_ref, kv_ref, s_scr, p_scr, sems):
    rows = q_ref.shape[0]
    steps = kv_ref.shape[0]
    tokens = s_scr.shape[1]
    loads = {}
    for g in range(steps):
        ends = [*range(0, tokens + 1, CHUNK), kv_ref.shape[1]]
        for n, at in enumerate(slice(*pair) for pair in zip(ends, ends[1:])):
            loads[n, g] = pltpu.make_async_copy(kv_hbm.at[g, at], kv_ref.at[g, at], sems.at[n, g])
            loads[n, g].start()
    slots = HD // 2
    me, core = pos_ref[0], pos_ref[1]
    partner = me + 1 - 2 * core
    holder = q_ref[:, HALF : HALF + HD].astype(f32)
    slot = q_ref[:, HALF + HD : HALF + 2 * HD].astype(f32)
    lane = lax.broadcasted_iota(jnp.int32, (rows, HD), 1)
    lane_slot = jnp.where(lane < slots, lane, lane - slots).astype(f32)

    def bias_of(device):
        hit = holder == device.astype(f32)
        first = jnp.min(jnp.where(hit, slot, 999.0), axis=1, keepdims=True)
        last = jnp.max(jnp.where(hit, slot, -1.0), axis=1, keepdims=True)
        count = jnp.sum(jnp.where(hit, 1.0, 0.0), axis=1, keepdims=True)
        used = (lane_slot == first) | (lane_slot == last)
        double = used & (first == last) & (count > 1.5)
        return jnp.where(used, jnp.where(double, BIAS, 0.0), UNUSED)

    bias = jnp.where(lane < slots, bias_of(me), bias_of(partner)).astype(bf16)

    pairs = steps * GROUPS // 2
    chunk = CHUNK
    chunks = tokens // chunk
    queries, peaks, outs = {}, {}, {}
    for i in range(pairs + 2):
        if i < pairs:
            heads = [q_ref[:, (2 * i + j) * HD : (2 * i + j + 1) * HD] for j in range(2)]
            queries[i] = jnp.concatenate([jnp.concatenate([q, bias], axis=1) for q in heads], axis=0)
            peaks[i] = None
        if 0 <= i - 2 and 2 * (i - 2) % GROUPS == 0:
            loads[chunks, 2 * (i - 2) // GROUPS].wait()
        if 0 <= i - 1 < pairs:
            top = jnp.max(peaks[i - 1], axis=0, keepdims=True).astype(bf16)
            peaks[i - 1] = top.astype(f32)
        for k in range(chunks):
            at = slice(k * chunk, (k + 1) * chunk)
            if i < pairs:
                if 2 * i % GROUPS == 0:
                    loads[k, 2 * i // GROUPS].wait()
                s = lax.dot_general(
                    kv_ref[2 * i // GROUPS, at, :], queries[i], (((1,), (1,)), ((), ())), preferred_element_type=f32
                )
                s_scr[i % 2, at, :] = s
                peak = jnp.max(s.reshape(chunk // 8, 8, 2 * rows), axis=0)
                peaks[i] = peak if peaks[i] is None else jnp.maximum(peaks[i], peak)
            if 0 <= i - 1 < pairs:
                n = i - 1
                p_scr[n % 2, at, :] = jnp.exp2((s_scr[n % 2, at, :] - peaks[n]) * RATE).astype(bf16)
            if 0 <= i - 2:
                n = i - 2
                tiles = [
                    kv_ref[2 * n // GROUPS, tokens + j * VROWS : tokens + (j + 1) * VROWS, :]
                    for j in range(k * chunk // TILE, (k + 1) * chunk // TILE)
                ]
                out = jnp.dot(jnp.concatenate(tiles, axis=1), p_scr[n % 2, at, :], preferred_element_type=f32)
                outs[n] = out if k == 0 else outs[n] + out
        if 0 <= i - 2:
            out = outs.pop(i - 2)
            for h in range(2):
                g, head = divmod(2 * (i - 2) + h, GROUPS)
                cols = slice(h * rows, (h + 1) * rows)
                stat = jnp.concatenate([peaks[i - 2][:, cols], out[HD : HD + 1, cols]], axis=0).astype(bf16)
                for j in range(4):
                    dest = dest_of(g, head, j)
                    for t in range(SLICE // 2):
                        pair = out[j * SLICE + 2 * t : j * SLICE + 2 * t + 2, cols]
                        out_ref[dest, :, t * rows : (t + 1) * rows] = pair.astype(bf16)
                    out_ref[dest, :, SLICE // 2 * rows :] = stat


def dest_of(g, h, j):
    return ((j % 2) * 4 + g * 2 + h // 4) * 8 + (h % 4) * 2 + j // 2


def merge_body(got_ref, out_ref):
    chips, _, _ = got_ref.shape
    rows = out_ref.shape[1]
    pairs = SLICE // 2
    stats = [got_ref[i, :, pairs * rows :].astype(f32) for i in range(chips)]
    top = functools.reduce(jnp.maximum, [s[:1] for s in stats])
    total = jnp.zeros((1, rows), f32)
    number = jnp.zeros((2, pairs * rows), f32)
    for i in range(chips):
        factor = jnp.exp2((stats[i][:1] - top) * RATE)
        total += factor * stats[i][1:]
        number += jnp.concatenate([factor] * pairs, axis=1) * got_ref[i, :, : pairs * rows].astype(f32)
    attention = number / jnp.concatenate([total] * pairs, axis=1)
    attention = jnp.concatenate([attention[:, t * rows : (t + 1) * rows] for t in range(pairs)], axis=0)
    high = attention.astype(bf16)
    out_ref[:SLICE, :] = high
    out_ref[SLICE:, :] = (attention - high.astype(f32)).astype(bf16)


def project_body(*refs):
    count = len(refs) // 2
    lefts, rights, out_ref = refs[:count], refs[count:-1], refs[-1]
    left = jnp.concatenate([r[...] for r in lefts], axis=0)
    step = 512
    for i in range(out_ref.shape[1] // step):
        cols = slice(i * step, (i + 1) * step)
        right = jnp.concatenate([r[:, cols] for r in rights for _ in range(2)], axis=0)
        part = lax.dot_general(left, right, (((0,), (0,)), ((), ())), preferred_element_type=f32)
        out_ref[:, cols] = part.astype(bf16)


def finish_body(got_ref, out_ref):
    devices, parts, part = got_ref.shape
    mates = out_ref.shape[1] // (parts * part)
    for m in range(mates):
        total = sum(got_ref[i].astype(f32) for i in range(m, devices, mates)).astype(bf16)
        for r in range(parts):
            at = (m * parts + r) * part
            out_ref[:, at : at + part] = total[r : r + 1]


def small_call(body, out, *args, scalars=(), scratch=(), mib=8, flops=0, large=0):
    smem = pl.BlockSpec(memory_space=pltpu.SMEM)
    vmem = pl.BlockSpec(memory_space=pltpu.VMEM)
    return pl.pallas_call(
        body,
        out_shape=out,
        in_specs=[smem] * len(scalars) + [vmem] * (len(args) - large) + [pl.BlockSpec(memory_space=pltpu.HBM)] * large,
        out_specs=jax.tree.map(lambda _: vmem, out),
        scratch_shapes=list(scratch),
        cost_estimate=pl.CostEstimate(flops=flops, transcendentals=0, bytes_accessed=0) if flops else None,
        compiler_params=pltpu.CompilerParams(vmem_limit_bytes=mib << 20),
        interpret=INTERPRET,
    )(*scalars, *args)


def swapped(v):
    return lax.ppermute(v, "c", [(0, 1), (1, 0)])


def to_mate(v, k):
    nx, nc = lax.axis_size("x"), lax.axis_size("c")
    perm = [(x * nc + c, (x ^ (k // nc)) * nc + (c ^ (k % nc))) for x in range(nx) for c in range(nc)]
    return lax.ppermute(v, ("x", "c"), perm)


def to_owner(v, k):
    ny, nx, nc = (lax.axis_size(a) for a in POOL)
    pairs = []
    for half in range(nc):
        for y in range(ny // nc):
            for x in range(nx):
                for c in range(nc):
                    source = ((half * (ny // nc) + y) * nx + x) * nc + c
                    target = ((c * (ny // nc) + y) * nx + (x ^ (k // nc))) * nc + (half ^ (k % nc))
                    pairs.append((source, target))
    return lax.ppermute(v, POOL, pairs)


def per_device(query, kv_pool, holder_table, slot_table, lengths, out_weight):
    ny, nx, nc = (lax.axis_size(a) for a in POOL)
    y, x, c = (lax.axis_index(a) for a in POOL)
    chips = ny * nx
    pos = jnp.stack([(y * nx + x) * nc + c, c]).astype(jnp.int32)

    devices = chips * nc
    width = HALF + 2 * holder_table.shape[1]
    row_shape = jax.ShapeDtypeStruct((devices, 2, width // 2), bf16)
    scratch = [pltpu.VMEM(v.shape, v.dtype) for v in (query, holder_table, slot_table)]
    rows = small_call(
        row_body,
        row_shape,
        query,
        holder_table,
        slot_table,
        scalars=(lengths,),
        scratch=[*scratch, pltpu.SemaphoreType.DMA((3,))],
        large=3,
        mib=62,
    )
    q = lax.all_to_all(rows, POOL, split_axis=0, concat_axis=0, tiled=True)

    kv_other = swapped(kv_pool)
    tokens = nc * kv_pool.shape[0] * kv_pool.shape[2]
    steps = KVH // nc
    kv_shape = (steps, tokens + tokens // TILE * VROWS, TILE)
    blocks = small_call(
        blocks_body, jax.ShapeDtypeStruct(kv_shape, bf16), kv_pool, kv_other, scalars=(pos,), flops=1 << 32
    )

    mates = 2 * nc
    first = (x % 2) * nc + y // (ny // nc)
    d_part = out_weight.shape[1] // mates
    weights = []
    for k in range(mates):
        part = lax.dynamic_slice_in_dim(out_weight, (first ^ k) * d_part, d_part, axis=1)
        weights.append(to_owner(part, k))

    q = q.reshape(devices, width)
    parts = small_call(
        attention_body,
        jax.ShapeDtypeStruct((chips, 2, (SLICE // 2 + 1) * devices), bf16),
        q,
        blocks,
        scalars=(pos,),
        scratch=[
            pltpu.VMEM(kv_shape, bf16),
            pltpu.VMEM((2, tokens, 2 * devices), f32),
            pltpu.VMEM((2, tokens, 2 * devices), bf16),
            pltpu.SemaphoreType.DMA((tokens // CHUNK + 1, steps)),
        ],
        mib=52,
        large=1,
        flops=1 << 34,
    )
    parts = lax.all_to_all(parts, CHIPS, split_axis=0, concat_axis=0, tiled=True)
    mine = small_call(merge_body, jax.ShapeDtypeStruct((2 * SLICE, devices), bf16), parts)
    lefts = [to_mate(mine, k) if k else mine for k in range(mates)]
    partial = small_call(project_body, jax.ShapeDtypeStruct((devices, d_part), bf16), *lefts, *weights)
    columns = lax.all_to_all(
        partial.reshape(devices, 2, d_part // 2), POOL, split_axis=0, concat_axis=0, tiled=True
    )
    return small_call(finish_body, jax.ShapeDtypeStruct((1, mates * d_part), bf16), columns)


def solution(mesh):
    torus = Mesh(mesh.devices.reshape(mesh.shape["grp"], 8, 8, 2), GRP_POOL)
    return jax.shard_map(
        per_device,
        mesh=torus,
        in_specs=(
            P(GRP_POOL, None),
            P(GRP_POOL, None, None, None),
            P(GRP_POOL, None),
            P(GRP_POOL, None),
            P(GRP_POOL),
            P(POOL, None),
        ),
        out_specs=P(GRP_POOL, None),
        check_vma=False,
    )
```
